512 devices in a mesh: rep: 16 (over y, z_lo), zero: 32 (over z_hi, x, core).
Axes of the slice: x: 4, y: 4, z: 16 (z_hi: 4, z_lo: 4; z = z_hi * 4 + z_lo), core: 2. Of those that a mesh axis runs over, the one named last changes fastest.
Arguments:
- pre_norm: bfloat16 [8192, 8192], P(('rep', 'zero')), may hold values from -6 to 6
- upstream: bfloat16 [8192, 8192], P(('rep', 'zero')), may hold values from -20 to 20
- norm_gain: float32 [8192], replicated, may hold values from 0.1 to 1.9
- saved_mean: float32 [8192], replicated, may hold values from -4 to 4
- inv_std: float32 [8192], replicated, may hold values from 0.5 to 1.5
- features: bfloat16 [401408, 512], P(('rep', 'zero')), may hold values from -24 to 24
- out_grads: bfloat16 [401408, 2048], P(('rep', 'zero')), may hold values from -24 to 24
Outputs:
- input_grad: bfloat16 [8192, 8192], P(('rep', 'zero'))
- gain_grad: float32 [8192], replicated
- bias_grad: float32 [8192], replicated
- weight_grad: float32 [512, 2048], P('zero')
The draws below stay inside these ranges and needn't reach their ends.
All inputs are finite; a program needn't handle non-finite values.
Results may differ from the reference program's by a relative error of at most 0.001.
Values sent between devices are 32-bit elements; how exact they have to be, the bound alone decides.
A program may use at most 64 MiB of HBM per device.

```python
import math
import jax
import jax.numpy as jnp
from jax import lax

F = 8192
CIN = 512
COUT = 2048
SPATIAL = 49
IMG_DEV = 16
IMAGES = 8192


def draw_upstream(key, part):
    key_noise, key_offset, key_perm, key_sign = jax.random.split(key, 4)
    devices = IMAGES // IMG_DEV
    row_device = jnp.arange(IMAGES) // IMG_DEV
    target = jax.random.permutation(key_perm, devices)[row_device]
    boosted = jnp.arange(F)[None, :] % devices == target[:, None]
    signs = jnp.where(jax.random.randint(key_sign, (devices,), 0, 2) == 0, -1.0, 1.0)[row_device]
    offset = 0.5 * jnp.clip(jax.random.normal(key_offset, (F,)), -4.0, 4.0)
    noise = jnp.clip(jax.random.normal(key_noise, (IMAGES, F)), -4.0, 4.0)
    values = offset[None, :] + noise + 4.0 * signs[:, None] * boosted.astype(jnp.float32)
    return jnp.clip(values, -20.0, 20.0).astype(jnp.float32).astype(jnp.bfloat16)


def raised(drawn, own_key, source, target, blocks, factor):
    owner, partner = [(jnp.arange(drawn.shape[axis_at]) // (drawn.shape[axis_at] // blocks)).reshape([-1 if axis == axis_at else 1 for axis in range(drawn.ndim)]) for axis_at in (source, target)]
    chosen = jax.random.permutation(own_key, blocks)[partner]
    strong = (owner == chosen) | (owner == (partner + blocks // 2) % blocks)
    return jnp.where(strong, factor * drawn, drawn)


def shard_levels(key, shape, cuts, smallest, largest):
    level, own = 1.0, jax.random.fold_in(key, 6)
    for position, blocks in cuts:
        steps = jnp.exp(jax.random.uniform(jax.random.fold_in(own, position), (blocks,), jnp.float32, smallest / len(cuts), largest / len(cuts)))
        level = level * jnp.repeat(steps, shape[position] // blocks).reshape([-1 if axis == position else 1 for axis in range(len(shape))])
    return level


def bell_draw(rng, shape, deviation, most, shards=(), held_as=jnp.bfloat16):
    result = deviation * jax.random.normal(rng, shape, jnp.float32)
    if shards:
        result = result * shard_levels(rng, shape, shards, -0.22, 0.18)
    return jnp.clip(result, -most, most).astype(held_as)


def gaussian_with(key, dims, spread, bound, shards, heavy, held_as=jnp.bfloat16):
    entries = spread * jax.random.normal(key, dims, jnp.float32)
    if shards:
        entries = entries * shard_levels(key, dims, shards, -0.22, 0.18)
    return jnp.clip(raised(entries, jax.random.fold_in(key, 3), *heavy), -bound, bound).astype(held_as)


def setup_inputs(seed: int = 0) -> dict:
    key_list = jax.random.split(jax.random.key(seed), 8)
    pre_norm = bell_draw(key_list[0], (IMAGES, F), 1.0, 6.0, ((0, 512),))
    upstream = draw_upstream(jax.random.fold_in(key_list[7], 71), 0)
    norm_gain = jnp.clip(1.0 + 0.18 * jax.random.normal(key_list[2], (F,), jnp.float32), 0.1, 1.9)
    saved_mean = bell_draw(key_list[3], (F,), 0.3, 4.0, (), jnp.float32)
    inv_std = jnp.clip(jnp.exp(jax.random.uniform(key_list[4], (F,), jnp.float32, math.log(0.5), math.log(1.5))), 0.5, 1.5)
    features = gaussian_with(key_list[5], (IMAGES * SPATIAL, CIN), 1.0, 24.0, ((0, 512),), (0, 1, 512, 6.0))
    out_grads = bell_draw(key_list[6], (IMAGES * SPATIAL, COUT), 4.0, 24.0, ((0, 512),))
    return {"pre_norm": pre_norm, "upstream": upstream, "norm_gain": norm_gain, "saved_mean": saved_mean, "inv_std": inv_std, "features": features, "out_grads": out_grads}


def reference(pre_norm, upstream, norm_gain, saved_mean, inv_std, features, out_grads):
    normed = (pre_norm.astype(jnp.float32) - saved_mean) * inv_std
    grads32 = upstream.astype(jnp.float32)
    bias_grad = jnp.sum(grads32, axis=0) / IMAGES
    gain_grad = jnp.sum(grads32 * normed, axis=0) / IMAGES
    input_grad = (norm_gain * inv_std * (grads32 - bias_grad - normed * gain_grad)).astype(jnp.bfloat16)
    blocks = IMAGES // IMG_DEV
    feat_blocks = features.reshape(blocks, IMG_DEV * SPATIAL, CIN)
    grad_blocks = out_grads.reshape(blocks, IMG_DEV * SPATIAL, COUT)

    def accumulate(total, pair):
        left, right = pair
        product = jnp.dot(left.astype(jnp.float32).T, right.astype(jnp.float32), precision=lax.Precision.HIGHEST)
        return total + product, None

    total, unused = lax.scan(accumulate, jnp.zeros((CIN, COUT), jnp.float32), (feat_blocks, grad_blocks))
    weight_grad = total / IMAGES
    return input_grad, gain_grad, bias_grad, weight_grad
```

```python
import functools

import jax
import jax.numpy as jnp
from jax import lax
from jax.experimental import pallas as pl
from jax.experimental.pallas import tpu as pltpu
from jax.sharding import PartitionSpec as P

MESH = pl.DeviceIdType.MESH
F = 8192
ROWS = 784
CIN = 512
COUT = 2048
IMAGES = 8192
NX, NY, NZL, NZH = 4, 4, 4, 4
NZ = NZL * NZH
W = 256
F_CORE, F_X, F_Y = F // 2, F // 8, F // 32


def mul(v, m):
    return pl.multiple_of(v, m)


class Copies:
    def __init__(self, send, recv):
        self.send, self.recv, self.n, self.all = send, recv, 0, []

    def make(self, src, dst, device):
        i = self.n
        self.n += 1
        copy = pltpu.make_async_remote_copy(
            src_ref=src,
            dst_ref=dst,
            send_sem=self.send.at[i],
            recv_sem=self.recv.at[i],
            device_id=device,
            device_id_type=MESH,
        )
        copy.start()
        self.all.append(copy)
        return copy


class Ring4:
    def __init__(self, copies, src, bufs, plus, minus):
        self.c, self.src, self.bufs, self.plus, self.minus = copies, src, bufs, plus, minus

    def send2(self):
        self.two_a = self.c.make(self.src(2, 0), self.bufs.at[0], self.plus)
        self.two_b = self.c.make(self.src(2, 1), self.bufs.at[1], self.minus)

    def direct_plus(self):
        self.dir_b = self.c.make(self.src(1, 1), self.bufs.at[3], self.plus)

    def direct_minus(self):
        self.dir_a = self.c.make(self.src(3, 0), self.bufs.at[2], self.minus)

    def acc_plus(self):
        self.two_a.wait_recv()
        ref = self.src(1, 0)
        ref[...] = ref[...] + self.bufs[0]
        self.acc_a = self.c.make(ref, self.bufs.at[4], self.plus)

    def acc_minus(self):
        self.two_b.wait_recv()
        ref = self.src(3, 1)
        ref[...] = ref[...] + self.bufs[1]
        self.acc_b = self.c.make(ref, self.bufs.at[5], self.minus)

    def final(self, half):
        direct, acc = (self.dir_a, self.acc_a) if half == 0 else (self.dir_b, self.acc_b)
        direct.wait_recv()
        acc.wait_recv()
        return self.src(0, half)[...] + self.bufs[2 + half] + self.bufs[4 + half]


def kernel(
    pre_h, up_h, gain_h, mean_h, inv_h, feat_h, og_h,
    ig_o, st_o, wg_o,
    pre, up, gain, mean, inv, feat, ft, og, ig,
    wp, wo, wd, x1, y1, x2, y2, zs, zr, wg,
    bnp, bnd, bnx, bny, bnz, bna, bnf,
    local_sem, send_sem, recv_sem, zsend, zrecv, bzsend, bzrecv, agsend, agrecv, zk,
):
    rep, zero = lax.axis_index("rep"), lax.axis_index("zero")
    y, zl = rep // NZL, lax.rem(rep, NZL)
    core = lax.rem(zero, 2)
    xq = zero // 2
    x, zh = lax.rem(xq, NX), xq // NX
    z = zh * NZL + zl

    def at(dx=0, dy=0, dz=0, dc=0):
        zz = lax.rem(z + dz + NZ, NZ)
        xx, yy = lax.rem(x + dx + NX, NX), lax.rem(y + dy + NY, NY)
        cc = lax.rem(core + dc, 2)
        return (yy * NZL + lax.rem(zz, NZL), (zz // NZL * NX + xx) * 2 + cc)

    loads = {}
    n_local = 0

    def load(name, src, dst):
        nonlocal n_local
        loads[name] = pltpu.make_async_copy(src, dst, local_sem.at[n_local])
        loads[name].start()
        n_local += 1

    load("up", up_h, up)
    load("pre", pre_h, pre)
    load("mean", mean_h, mean)
    load("inv", inv_h, inv)
    load("feat", feat_h, feat)
    offsets = (2, 1, 3, 0)
    for s in range(8):
        colour, k = s % 2, s // 2
        column = mul(colour * 1024 + lax.rem(y + offsets[k], NY) * W, W)
        load(("og", s), og_h.at[:, pl.ds(column, W)], og.at[s])
    load("gain", gain_h, gain)

    barrier = pltpu.get_barrier_semaphore()
    near = [at(dc=1), at(dz=1), at(dz=-1)]
    near += [at(dx=d) for d in (1, 2, 3)] + [at(dy=d) for d in (1, 2, 3)]
    for device in near:
        pl.semaphore_signal(barrier, inc=1, device_id=device, device_id_type=MESH)

    copies = Copies(send_sem, recv_sem)

    for name in ("up", "pre", "mean", "inv"):
        loads[name].wait()

    def sums(i, carry):
        cols = pl.ds(mul(i * 512, 512), 512)
        g = up[:, cols].astype(jnp.float32)
        n = (pre[:, cols].astype(jnp.float32) - mean[:, cols]) * inv[:, cols]
        bnp[0:1, cols] = jnp.sum(g, axis=0, keepdims=True)
        bnp[1:2, cols] = jnp.sum(g * n, axis=0, keepdims=True)
        return carry

    lax.fori_loop(0, F // 512, sums, 0)

    pl.semaphore_wait(barrier, len(near))

    def z_round(i, hop):
        for d in (hop, -hop):
            pl.semaphore_signal(zk.at[i], inc=1, device_id=at(dz=d), device_id_type=MESH)

    z_round(0, 1)

    mine = core * F_CORE
    other = (1 - core) * F_CORE
    bn_pair = copies.make(bnp.at[:, pl.ds(mul(other, F_CORE), F_CORE)], bnd, at(dc=1))

    loads["feat"].wait()
    t = feat[...].T
    for c in range(2):
        for xx in range(NX):
            for zz in range(NZH):
                dst = ((c * NX + xx) * NZH + zz) * 16
                src = ((zz * NX + xx) * 2 + c) * 16
                ft[dst : dst + 16, :] = t[src : src + 16, :]

    def product(s, c):
        left = ft[pl.ds(mul(c * 256, 256), 256), :]
        return lax.dot_general(
            left, og[s], (((1,), (0,)), ((), ())), preferred_element_type=jnp.float32
        )

    pair = []
    for s in range(8):
        loads[("og", s)].wait()
        wp[s] = product(s, 1 - core)
        pair.append(copies.make(wp.at[s], wd.at[s], at(dc=1)))

    bn_pair.wait_recv()
    half = pl.ds(mul(mine, F_CORE), F_CORE)
    bnp[:, half] = bnp[:, half] + bnd[...]

    def f_x(d):
        return pl.ds(mul(mine + lax.rem(x + d, NX) * F_X, F_X), F_X)

    bn_x = [copies.make(bnp.at[:, f_x(d)], bnx.at[d], at(dx=d)) for d in (2, 1, 3)]

    def wait_z_round(i):
        pl.semaphore_wait(zk.at[i], 2)

    wait_z_round(0)
    z_round(1, 2)

    def x_rows(xx, h, base=0):
        return pl.ds(mul(lax.rem(x + xx, NX) * 64 + h * 32, 32), 32)

    ring_x1 = [
        Ring4(
            copies,
            lambda off, h, k=k: wo.at[2 * k, x_rows(off, h)],
            x1.at[k],
            at(dx=1),
            at(dx=-1),
        )
        for k in range(4)
    ]
    order = {2: 0, 1: 1, 3: 2, 0: 3}
    ring_y1 = [
        Ring4(
            copies,
            lambda off, h, p=p: wo.at[2 * order[off] + 1, p * 128 + h * 64 : p * 128 + h * 64 + 64],
            y1.at[p],
            at(dy=1),
            at(dy=-1),
        )
        for p in range(2)
    ]
    for s in range(8):
        colour, k = s % 2, s // 2
        own = product(s, core)
        pair[s].wait_recv()
        wo[s] = own + wd[s]
        if colour == 0:
            ring_x1[k].send2()
        else:
            for ring in ring_y1:
                if k == 0:
                    ring.send2()
                elif k == 1:
                    ring.direct_plus()
                elif k == 2:
                    ring.direct_minus()

    for c in bn_x:
        c.wait_recv()
    mine_x = f_x(0)
    bnp[:, mine_x] = bnp[:, mine_x] + bnx[1] + bnx[2] + bnx[3]

    def f_y(d):
        return pl.ds(mul(mine + x * F_X + lax.rem(y + d, NY) * F_Y, F_Y), F_Y)

    bn_y = [copies.make(bnp.at[:, f_y(d)], bny.at[d], at(dy=d)) for d in (2, 1, 3)]
    wait_z_round(1)
    z_round(2, 4)

    def acc_x(k):
        ring_x1[k].acc_plus()
        ring_x1[k].acc_minus()
        ring_x1[k].direct_plus()
        ring_x1[k].direct_minus()

    def acc_y(p):
        ring_y1[p].acc_plus()
        ring_y1[p].acc_minus()

    acc_x(0)
    acc_x(1)
    acc_y(0)
    acc_x(2)
    acc_x(3)
    acc_y(1)

    for c in bn_y:
        c.wait_recv()
    wait_z_round(2)
    bnz[z] = bnp[:, f_y(0)] + bny[1] + bny[2] + bny[3]
    far = [8, 7, 9, 6, 10, 5, 11, 4, 12, 3, 13, 2, 14, 1, 15]

    def bz_copy(i, d):
        return pltpu.make_async_remote_copy(
            src_ref=bnz.at[z],
            dst_ref=bnz.at[z],
            send_sem=bzsend.at[i],
            recv_sem=bzrecv.at[i],
            device_id=at(dz=d),
            device_id_type=MESH,
        )

    def bz_arrival(i, d):
        slot = lax.rem(z - d + NZ, NZ)
        return pltpu.make_async_remote_copy(
            src_ref=bnz.at[slot],
            dst_ref=bnz.at[slot],
            send_sem=bzsend.at[i],
            recv_sem=bzrecv.at[i],
            device_id=at(dz=d),
            device_id_type=MESH,
        )

    for i, d in enumerate(far):
        bz_copy(i, d).start()

    ring_x2 = Ring4(
        copies,
        lambda off, h: wo.at[2 * order[off], x_rows(0, h)],
        x2,
        at(dy=1),
        at(dy=-1),
    )
    ring_y2 = Ring4(copies, lambda off, h: wo.at[7, x_rows(off, h)], y2, at(dx=1), at(dx=-1))

    def final_x(k):
        for h in range(2):
            wo[2 * k, x_rows(0, h)] = ring_x1[k].final(h)

    def final_y(p):
        for h in range(2):
            rows = p * 128 + h * 64
            wo[7, rows : rows + 64] = ring_y1[p].final(h)

    final_x(0)
    ring_x2.send2()
    final_x(1)
    ring_x2.direct_plus()
    final_x(2)
    ring_x2.direct_minus()
    final_y(0)
    final_y(1)
    ring_y2.send2()
    ring_y2.direct_plus()
    ring_y2.direct_minus()
    final_x(3)
    ring_x2.acc_plus()
    ring_x2.acc_minus()

    for i, d in enumerate(far):
        bz_arrival(i, d).wait_recv()
    total = bnz[0]
    for i in range(1, NZ):
        total = total + bnz[i]
    bna[:, f_y(0)] = total * (1.0 / IMAGES)
    bn_ay = [copies.make(bna.at[:, f_y(0)], bna.at[:, f_y(0)], at(dy=d)) for d in (2, 1, 3)]

    ring_y2.acc_plus()
    ring_y2.acc_minus()

    def wgt_z(colour):
        ring = ring_x2 if colour == 0 else ring_y2
        for h in range(2):
            v = ring.final(h)
            for i in range(2):
                zs[2 * colour + i, h * 32 : h * 32 + 32, :] = v[:, i * 128 : i * 128 + 128]

    def z_piece(d):
        zz = lax.rem(z + d, NZ)
        return zs.at[lax.rem(zz, NZL), pl.ds(mul(zz // NZL * 16, 16), 16)]

    def z_copy(i, d):
        return pltpu.make_async_remote_copy(
            src_ref=z_piece(d),
            dst_ref=zr.at[d],
            send_sem=zsend.at[i],
            recv_sem=zrecv.at[i],
            device_id=at(dz=d),
            device_id_type=MESH,
        )

    wgt_z(0)
    wgt_z(1)
    z_copies = [z_copy(i, d) for i, d in enumerate(far)]
    for c in z_copies:
        c.start()

    for i, d in enumerate((2, 1, 3)):
        bn_ay[i].wait_recv()
    bn_ax = [copies.make(bna.at[:, f_x(0)], bna.at[:, f_x(0)], at(dx=d)) for d in (2, 1, 3)]
    for c in bn_ax:
        c.wait_recv()
    bn_ap = copies.make(bna.at[:, half], bna.at[:, half], at(dc=1))
    bn_ap.wait_recv()
    loads["gain"].wait()

    def grads(i, carry):
        cols = pl.ds(mul(i * 512, 512), 512)
        g = up[:, cols].astype(jnp.float32)
        n = (pre[:, cols].astype(jnp.float32) - mean[:, cols]) * inv[:, cols]
        scale = gain[:, cols] * inv[:, cols]
        ig[:, cols] = (scale * (g - bna[0:1, cols] - n * bna[1:2, cols])).astype(jnp.bfloat16)
        return carry

    lax.fori_loop(0, F // 512, grads, 0)
    ig_store = pltpu.make_async_copy(ig, ig_o, local_sem.at[n_local])
    ig_store.start()
    st_store = pltpu.make_async_copy(bna, st_o, local_sem.at[n_local + 1])
    st_store.start()

    result = zs[zl, pl.ds(mul(zh * 16, 16), 16)]
    for i, d in enumerate(far):
        z_copies[i].wait_recv()
        result = result + zr[d]
    column = mul(zl // 2 * 1024 + y * W + lax.rem(zl, 2) * 128, 128)
    wg[:, pl.ds(column, 128)] = result * (1.0 / IMAGES)

    peers = [(2, 3), (2, 1), (2, 2), (1, 3), (3, 3), (1, 1), (3, 1), (1, 2), (3, 2), (2, 0), (0, 3), (0, 1), (0, 2), (1, 0), (3, 0)]

    def ag_copy(i, dy, dl, sent):
        yy, ll = (lax.rem(y + dy, NY), lax.rem(zl + dl, NZL))
        sy, sl = (y, zl) if sent else (lax.rem(y - dy + NY, NY), lax.rem(zl - dl + NZL, NZL))
        ref = wg.at[:, pl.ds(mul(sl // 2 * 1024 + sy * W + lax.rem(sl, 2) * 128, 128), 128)]
        return pltpu.make_async_remote_copy(
            src_ref=ref,
            dst_ref=ref,
            send_sem=agsend.at[i],
            recv_sem=agrecv.at[i],
            device_id=(yy * NZL + ll, zero),
            device_id_type=MESH,
        )

    for i, (dy, dl) in enumerate(peers):
        ag_copy(i, dy, dl, True).start()
    for i, (dy, dl) in enumerate(peers):
        ag_copy(i, dy, dl, False).wait_recv()
    wg_store = pltpu.make_async_copy(wg, wg_o, local_sem.at[n_local + 2])
    wg_store.start()

    for c in copies.all:
        c.wait_send()
    for i, d in enumerate(far):
        z_copies[i].wait_send()
        bz_copy(i, d).wait_send()
    for i, (dy, dl) in enumerate(peers):
        ag_copy(i, dy, dl, True).wait_send()
    ig_store.wait()
    st_store.wait()
    wg_store.wait()


N_COPIES = 96


def per_device(pre_norm, upstream, norm_gain, saved_mean, inv_std, features, out_grads):
    row = lambda v: v.reshape(1, F)
    f32, bf16 = jnp.float32, jnp.bfloat16
    vm = pltpu.VMEM
    dma = pltpu.SemaphoreType.DMA
    ig, st, wg = pl.pallas_call(
        kernel,
        out_shape=(
            jax.ShapeDtypeStruct((16, F), bf16),
            jax.ShapeDtypeStruct((2, F), f32),
            jax.ShapeDtypeStruct((16, COUT), f32),
        ),
        in_specs=[pl.BlockSpec(memory_space=pl.ANY)] * 7,
        out_specs=(pl.BlockSpec(memory_space=pl.ANY),) * 3,
        scratch_shapes=[
            vm((16, F), bf16), vm((16, F), bf16), vm((1, F), f32), vm((1, F), f32), vm((1, F), f32),
            vm((ROWS, CIN), bf16), vm((CIN, ROWS), bf16), vm((8, ROWS, W), bf16), vm((16, F), bf16),
            vm((8, 256, W), f32), vm((8, 256, W), f32), vm((8, 256, W), f32),
            vm((4, 6, 32, W), f32), vm((2, 6, 64, W), f32), vm((6, 32, W), f32), vm((6, 32, W), f32),
            vm((NZL, 64, 128), f32), vm((NZ, 16, 128), f32), vm((16, COUT), f32),
            vm((2, F), f32), vm((2, F_CORE), f32), vm((4, 2, F_X), f32), vm((4, 2, F_Y), f32),
            vm((NZ, 2, F_Y), f32), vm((2, F), f32), vm((8, 128), f32),
            dma((17,)), dma((N_COPIES,)), dma((N_COPIES,)),
            dma((15,)), dma((15,)), dma((15,)), dma((15,)), dma((15,)), dma((15,)),
            pltpu.SemaphoreType.REGULAR((3,)),
        ],
        compiler_params=pltpu.CompilerParams(
            collective_id=0, has_side_effects=True, vmem_limit_bytes=48 * 1024 * 1024
        ),
        name="twins",
    )(pre_norm, upstream, row(norm_gain), row(saved_mean), row(inv_std), features, out_grads)
    return ig, st[1], st[0], wg


def solution(mesh):
    split = P(("rep", "zero"), None)
    return jax.shard_map(
        per_device,
        mesh=mesh,
        in_specs=(split, split, P(), P(), P(), split, split),
        out_specs=(split, P(), P(), P("zero", None)),
        check_vma=False,
    )
```

```python
import functools

import jax
import jax.numpy as jnp
from jax import lax
from jax.experimental import pallas as pl
from jax.experimental.pallas import tpu as pltpu
from jax.sharding import PartitionSpec as P

MESH = pl.DeviceIdType.MESH
F = 8192
ROWS = 784
CIN = 512
COUT = 2048
IMAGES = 8192
NX, NY, NZL, NZH = 4, 4, 4, 4
NZ = NZL * NZH
W = 256
F_CORE, F_X, F_Y = F // 2, F // 8, F // 32


def mul(v, m):
    return pl.multiple_of(v, m)


class Phases:
    def __init__(self):
        self.open = None

    def __call__(self, name):
        if self.open is not None:
            self.open.__exit__(None, None, None)
        self.open = None
        if name is not None:
            self.open = jax.named_scope(name)
            self.open.__enter__()


class Copies:
    def __init__(self, send, recv):
        self.send, self.recv, self.n, self.all = send, recv, 0, []

    def make(self, src, dst, device):
        i = self.n
        self.n += 1
        copy = pltpu.make_async_remote_copy(
            src_ref=src,
            dst_ref=dst,
            send_sem=self.send.at[i],
            recv_sem=self.recv.at[i],
            device_id=device,
            device_id_type=MESH,
        )
        copy.start()
        self.all.append(copy)
        return copy


class Ring4:
    def __init__(self, copies, src, bufs, plus, minus):
        self.c, self.src, self.bufs, self.plus, self.minus = copies, src, bufs, plus, minus

    def send2(self):
        self.two_a = self.c.make(self.src(2, 0), self.bufs.at[0], self.plus)
        self.two_b = self.c.make(self.src(2, 1), self.bufs.at[1], self.minus)

    def direct_plus(self):
        self.dir_b = self.c.make(self.src(1, 1), self.bufs.at[3], self.plus)

    def direct_minus(self):
        self.dir_a = self.c.make(self.src(3, 0), self.bufs.at[2], self.minus)

    def acc_plus(self):
        self.two_a.wait_recv()
        ref = self.src(1, 0)
        ref[...] = ref[...] + self.bufs[0]
        self.acc_a = self.c.make(ref, self.bufs.at[4], self.plus)

    def acc_minus(self):
        self.two_b.wait_recv()
        ref = self.src(3, 1)
        ref[...] = ref[...] + self.bufs[1]
        self.acc_b = self.c.make(ref, self.bufs.at[5], self.minus)

    def final(self, half):
        direct, acc = (self.dir_a, self.acc_a) if half == 0 else (self.dir_b, self.acc_b)
        direct.wait_recv()
        acc.wait_recv()
        return self.src(0, half)[...] + self.bufs[2 + half] + self.bufs[4 + half]


def kernel(
    pre_h, up_h, gain_h, mean_h, inv_h, feat_h, og_h,
    ig, gain_o, bias_o, wg,
    pre, up, gain, mean, inv, feat, ft, og,
    wp, wo, wd, x1, y1, x2, y2, zs, zr,
    bnp, bnd, bnx, bnz, bna,
    local_sem, send_sem, recv_sem, zsend, zrecv, bzsend, bzrecv, agsend, agrecv, zk,
):
    rep, zero = lax.axis_index("rep"), lax.axis_index("zero")
    y, zl = rep // NZL, lax.rem(rep, NZL)
    core = lax.rem(zero, 2)
    xq = zero // 2
    x, zh = lax.rem(xq, NX), xq // NX
    z = zh * NZL + zl

    def at(dx=0, dy=0, dz=0, dc=0):
        zz = lax.rem(z + dz + NZ, NZ)
        xx, yy = lax.rem(x + dx + NX, NX), lax.rem(y + dy + NY, NY)
        cc = lax.rem(core + dc, 2)
        return (yy * NZL + lax.rem(zz, NZL), (zz // NZL * NX + xx) * 2 + cc)

    phase = Phases()
    phase("start")
    loads = {}
    n_local = 0

    def load(name, src, dst):
        nonlocal n_local
        loads[name] = pltpu.make_async_copy(src, dst, local_sem.at[n_local])
        loads[name].start()
        n_local += 1

    load("feat", feat_h, feat)
    load("up", up_h, up)
    load("pre", pre_h, pre)
    load("mean", mean_h, mean)
    load("inv", inv_h, inv)
    offsets = (2, 1, 3, 0)
    for s in range(8):
        colour, k = s % 2, s // 2
        column = mul(colour * 1024 + lax.rem(y + offsets[k], NY) * W, W)
        load(
            ("og", s),
            og_h.at[:, pl.ds(column, W)],
            og.at[s // 4, :, s % 4 * W : s % 4 * W + W],
        )
    load("gain", gain_h, gain)

    barrier = pltpu.get_barrier_semaphore()
    plane = [(2, 2), (2, 1), (2, 3), (1, 2), (3, 2), (1, 1), (1, 3), (3, 1), (3, 3)]
    plane += [(2, 0), (0, 2), (1, 0), (3, 0), (0, 1), (0, 3)]
    near = [at(dc=1), at(dz=1), at(dz=-1)] + [at(dx=dx, dy=dy) for dx, dy in plane]
    for device in near:
        pl.semaphore_signal(barrier, inc=1, device_id=device, device_id_type=MESH)

    copies = Copies(send_sem, recv_sem)

    phase("featwait")
    loads["feat"].wait()
    phase("transpose")
    t = feat[...].T
    for c in range(2):
        for xx in range(NX):
            for zz in range(NZH):
                dst = ((c * NX + xx) * NZH + zz) * 16
                src = ((zz * NX + xx) * 2 + c) * 16
                ft[dst : dst + 16, :] = t[src : src + 16, :]

    phase("bnload")
    for name in ("up", "pre", "mean", "inv"):
        loads[name].wait()

    phase("bnsum")
    def sums(i, carry):
        cols = pl.ds(mul(i * 512, 512), 512)
        g = up[:, cols].astype(jnp.float32)
        n = (pre[:, cols].astype(jnp.float32) - mean[:, cols]) * inv[:, cols]
        bnp[0:1, cols] = jnp.sum(g, axis=0, keepdims=True)
        bnp[1:2, cols] = jnp.sum(g * n, axis=0, keepdims=True)
        return carry

    lax.fori_loop(0, F // 512, sums, 0)

    phase("barrier")
    pl.semaphore_wait(barrier, len(near))

    def z_round(i, hop):
        for d in (hop, -hop):
            pl.semaphore_signal(zk.at[i], inc=1, device_id=at(dz=d), device_id_type=MESH)

    z_round(0, 1)

    mine = core * F_CORE
    other = (1 - core) * F_CORE
    bn_pair = copies.make(bnp.at[:, pl.ds(mul(other, F_CORE), F_CORE)], bnd, at(dc=1))

    phase("products")
    def product(part, c, out):
        left = ft[pl.ds(mul(c * 256, 256), 256), :]
        v = lax.dot_general(
            left, og[part], (((1,), (0,)), ((), ())), preferred_element_type=jnp.float32
        )
        for i in range(4):
            out[4 * part + i] = v[:, i * W : i * W + W]

    pair = []
    for part in range(2):
        for i in range(4):
            loads[("og", 4 * part + i)].wait()
        product(part, 1 - core, wp)
        for i in range(4):
            s = 4 * part + i
            pair.append(copies.make(wp.at[s], wd.at[s], at(dc=1)))

    phase("bnpair")
    bn_pair.wait_recv()
    half = pl.ds(mul(mine, F_CORE), F_CORE)
    bnp[:, half] = bnp[:, half] + bnd[...]

    def f_xy(dx, dy):
        start = mine + lax.rem(x + dx, NX) * F_X + lax.rem(y + dy, NY) * F_Y
        return pl.ds(mul(start, F_Y), F_Y)

    bn_xy = [
        copies.make(bnp.at[:, f_xy(dx, dy)], bnx.at[4 * dx + dy], at(dx=dx, dy=dy))
        for dx, dy in plane
    ]

    def wait_z_round(i):
        pl.semaphore_wait(zk.at[i], 2)

    wait_z_round(0)
    z_round(1, 2)

    phase("own")
    def x_rows(xx, h, base=0):
        return pl.ds(mul(lax.rem(x + xx, NX) * 64 + h * 32, 32), 32)

    ring_x1 = [
        Ring4(
            copies,
            lambda off, h, k=k: wo.at[2 * k, x_rows(off, h)],
            x1.at[k],
            at(dx=1),
            at(dx=-1),
        )
        for k in range(4)
    ]
    order = {2: 0, 1: 1, 3: 2, 0: 3}
    ring_y1 = [
        Ring4(
            copies,
            lambda off, h, p=p: wo.at[2 * order[off] + 1, p * 128 + h * 64 : p * 128 + h * 64 + 64],
            y1.at[p],
            at(dy=1),
            at(dy=-1),
        )
        for p in range(2)
    ]
    for s in range(8):
        colour, k = s % 2, s // 2
        if s % 4 == 0:
            phase(f"own{s // 4}")
            product(s // 4, core, wo)
        phase(f"pairwait{s}")
        pair[s].wait_recv()
        phase(f"add{s}")
        wo[s] = wo[s] + wd[s]
        if colour == 0:
            ring_x1[k].send2()
        else:
            for ring in ring_y1:
                if k == 0:
                    ring.send2()
                elif k == 1:
                    ring.direct_plus()
                elif k == 2:
                    ring.direct_minus()
    wait_z_round(1)
    z_round(2, 4)

    def acc_x(k):
        ring_x1[k].acc_plus()
        ring_x1[k].acc_minus()
        ring_x1[k].direct_plus()
        ring_x1[k].direct_minus()

    def acc_y(p):
        ring_y1[p].acc_plus()
        ring_y1[p].acc_minus()

    phase("accx0")
    acc_x(0)
    phase("accx1")
    acc_x(1)
    phase("bnxy")
    for c in bn_xy:
        c.wait_recv()
    wait_z_round(2)
    total = bnp[:, f_xy(0, 0)]
    for dx, dy in plane:
        total = total + bnx[4 * dx + dy]
    bnz[z] = total
    far = [8, 7, 9, 6, 10, 5, 11, 4, 12, 3, 13, 2, 14, 1, 15]

    def bz_copy(i, d):
        return pltpu.make_async_remote_copy(
            src_ref=bnz.at[z],
            dst_ref=bnz.at[z],
            send_sem=bzsend.at[i],
            recv_sem=bzrecv.at[i],
            device_id=at(dz=d),
            device_id_type=MESH,
        )

    def bz_arrival(i, d):
        slot = lax.rem(z - d + NZ, NZ)
        return pltpu.make_async_remote_copy(
            src_ref=bnz.at[slot],
            dst_ref=bnz.at[slot],
            send_sem=bzsend.at[i],
            recv_sem=bzrecv.at[i],
            device_id=at(dz=d),
            device_id_type=MESH,
        )

    for i, d in enumerate(far):
        bz_copy(i, d).start()

    phase("accy0")
    acc_y(0)
    phase("accx2")
    acc_x(2)
    phase("accx3")
    acc_x(3)
    phase("accy1")
    acc_y(1)

    ring_x2 = Ring4(
        copies,
        lambda off, h: wo.at[2 * order[off], x_rows(0, h)],
        x2,
        at(dy=1),
        at(dy=-1),
    )
    ring_y2 = Ring4(copies, lambda off, h: wo.at[7, x_rows(off, h)], y2, at(dx=1), at(dx=-1))

    def final_x(k):
        for h in range(2):
            wo[2 * k, x_rows(0, h)] = ring_x1[k].final(h)

    def final_y(p):
        for h in range(2):
            rows = p * 128 + h * 64
            wo[7, rows : rows + 64] = ring_y1[p].final(h)

    phase("finx0")
    final_x(0)
    ring_x2.send2()
    phase("finx1")
    final_x(1)
    ring_x2.direct_plus()
    phase("finx2")
    final_x(2)
    ring_x2.direct_minus()
    phase("finy0")
    final_y(0)
    phase("finy1")
    final_y(1)
    ring_y2.send2()
    ring_y2.direct_plus()
    ring_y2.direct_minus()
    phase("finx3")
    final_x(3)
    phase("accx2s")
    ring_x2.acc_plus()
    ring_x2.acc_minus()

    def z_copy(colour, j):
        ll = 2 * colour + j % 2
        hh = lax.rem(zh + offsets[j // 2], NZH)
        copy = pltpu.make_async_remote_copy(
            src_ref=zs.at[ll, pl.ds(mul(hh * 16, 16), 16)],
            dst_ref=zr.at[z],
            send_sem=zsend.at[8 * colour + j],
            recv_sem=zrecv.at[z],
            device_id=(y * NZL + ll, (hh * NX + x) * 2 + core),
            device_id_type=MESH,
        )
        return copy, (None if j < 6 else ll != zl)

    def each_z(colour, act):
        for j in range(8):
            copy, guard = z_copy(colour, j)
            if guard is None:
                act(copy)
            else:
                pl.when(guard)(lambda copy=copy: act(copy))

    def weight_z(colour):
        ring = ring_x2 if colour == 0 else ring_y2
        for h in range(2):
            v = ring.final(h)
            for i in range(2):
                zs[2 * colour + i, h * 32 : h * 32 + 32, :] = v[:, i * 128 : i * 128 + 128]
        each_z(colour, lambda copy: copy.start())

    phase("wgtz0")
    weight_z(0)
    phase("accy2s")
    ring_y2.acc_plus()
    ring_y2.acc_minus()
    phase("bnz")
    for i, d in enumerate(far):
        bz_arrival(i, d).wait_recv()
    total = bnz[0]
    for i in range(1, NZ):
        total = total + bnz[i]
    bna[:, f_xy(0, 0)] = total * (1.0 / IMAGES)
    bn_axy = [
        copies.make(bna.at[:, f_xy(0, 0)], bna.at[:, f_xy(0, 0)], at(dx=dx, dy=dy))
        for dx, dy in plane
    ]

    phase("wgtz1")
    weight_z(1)

    phase("bngxy")
    for i, (dx, dy) in enumerate(plane):
        bn_axy[i].wait_recv()
    bn_ap = copies.make(bna.at[:, half], bna.at[:, half], at(dc=1))

    phase("zwait")
    result = zs[zl, pl.ds(mul(zh * 16, 16), 16)]
    for d in far:
        slot = lax.rem(z - d + NZ, NZ)
        pltpu.make_async_remote_copy(
            src_ref=zr.at[slot],
            dst_ref=zr.at[slot],
            send_sem=zsend.at[0],
            recv_sem=zrecv.at[slot],
            device_id=at(dz=d),
            device_id_type=MESH,
        ).wait_recv()
        result = result + zr[slot]
    column = mul(zl // 2 * 1024 + y * W + lax.rem(zl, 2) * 128, 128)
    wg[:, pl.ds(column, 128)] = result * (1.0 / IMAGES)

    phase("ag")
    peers = [(2, 3), (2, 1), (2, 2), (1, 3), (3, 3), (1, 1), (3, 1), (1, 2), (3, 2), (2, 0), (0, 3), (0, 1), (0, 2), (1, 0), (3, 0)]

    def ag_copy(i, dy, dl, sent):
        yy, ll = (lax.rem(y + dy, NY), lax.rem(zl + dl, NZL))
        sy, sl = (y, zl) if sent else (lax.rem(y - dy + NY, NY), lax.rem(zl - dl + NZL, NZL))
        ref = wg.at[:, pl.ds(mul(sl // 2 * 1024 + sy * W + lax.rem(sl, 2) * 128, 128), 128)]
        return pltpu.make_async_remote_copy(
            src_ref=ref,
            dst_ref=ref,
            send_sem=agsend.at[i],
            recv_sem=agrecv.at[i],
            device_id=(yy * NZL + ll, zero),
            device_id_type=MESH,
        )

    for i, (dy, dl) in enumerate(peers):
        ag_copy(i, dy, dl, True).start()
    phase("bngp")
    bn_ap.wait_recv()
    loads["gain"].wait()
    phase("grads")

    def grads(i, carry):
        cols = pl.ds(mul(i * 512, 512), 512)
        g = up[:, cols].astype(jnp.float32)
        n = (pre[:, cols].astype(jnp.float32) - mean[:, cols]) * inv[:, cols]
        scale = gain[:, cols] * inv[:, cols]
        bias_grad, gain_grad = bna[0:1, cols], bna[1:2, cols]
        bias_o[:, cols] = bias_grad
        gain_o[:, cols] = gain_grad
        ig[:, cols] = (scale * (g - bias_grad - n * gain_grad)).astype(jnp.bfloat16)
        return carry

    lax.fori_loop(0, F // 512, grads, 0)
    phase("agwait")
    for i, (dy, dl) in enumerate(peers):
        ag_copy(i, dy, dl, False).wait_recv()
    phase("drain")
    for c in copies.all:
        c.wait_send()
    for colour in range(2):
        each_z(colour, lambda copy: copy.wait_send())
    for i, d in enumerate(far):
        bz_copy(i, d).wait_send()
    for i, (dy, dl) in enumerate(peers):
        ag_copy(i, dy, dl, True).wait_send()
    phase(None)


N_COPIES = 96


def store(ig, gain, bias, wg, ig_o, gain_o, bias_o, wg_o, sem):
    pairs = ((ig, ig_o), (wg, wg_o), (gain, gain_o), (bias, bias_o))
    copies = [pltpu.make_async_copy(a, b, sem.at[i]) for i, (a, b) in enumerate(pairs)]
    for copy in copies:
        copy.start()
    for copy in copies:
        copy.wait()


def per_device(pre_norm, upstream, norm_gain, saved_mean, inv_std, features, out_grads):
    row = lambda v: v.reshape(1, F)
    f32, bf16 = jnp.float32, jnp.bfloat16
    vm = pltpu.VMEM
    dma = pltpu.SemaphoreType.DMA
    outs = (
        jax.ShapeDtypeStruct((16, F), bf16),
        jax.ShapeDtypeStruct((1, F), f32),
        jax.ShapeDtypeStruct((1, F), f32),
        jax.ShapeDtypeStruct((16, COUT), f32),
    )
    vectors = (row(norm_gain), row(saved_mean), row(inv_std))
    arrays = (pre_norm, upstream, *vectors, features, out_grads)
    results = pl.pallas_call(
        kernel,
        out_shape=outs,
        in_specs=[pl.BlockSpec(memory_space=pltpu.HBM)] * 7,
        out_specs=(pl.BlockSpec(memory_space=vm),) * 4,
        scratch_shapes=[
            vm((16, F), bf16), vm((16, F), bf16), vm((1, F), f32), vm((1, F), f32), vm((1, F), f32),
            vm((ROWS, CIN), bf16), vm((CIN, ROWS), bf16), vm((2, ROWS, 4 * W), bf16),
            vm((8, 256, W), f32), vm((8, 256, W), f32), vm((8, 256, W), f32),
            vm((4, 6, 32, W), f32), vm((2, 6, 64, W), f32), vm((6, 32, W), f32), vm((6, 32, W), f32),
            vm((NZL, 64, 128), f32), vm((NZ, 16, 128), f32),
            vm((2, F), f32), vm((2, F_CORE), f32), vm((16, 2, F_Y), f32),
            vm((NZ, 2, F_Y), f32), vm((2, F), f32),
            dma((14,)), dma((N_COPIES,)), dma((N_COPIES,)),
            dma((16,)), dma((16,)), dma((15,)), dma((15,)), dma((15,)), dma((15,)),
            pltpu.SemaphoreType.REGULAR((3,)),
        ],
        compiler_params=pltpu.CompilerParams(
            collective_id=0, has_side_effects=True, vmem_limit_bytes=32 * 1024 * 1024
        ),
        name="twins",
    )(*(pltpu.with_memory_space_constraint(v, pltpu.HBM) for v in arrays))
    ig, gain_grad, bias_grad, wg = pl.pallas_call(
        store,
        out_shape=outs,
        in_specs=[pl.BlockSpec(memory_space=pl.ANY)] * 4,
        out_specs=(pl.BlockSpec(memory_space=pltpu.HBM),) * 4,
        scratch_shapes=[dma((4,))],
        name="store",
    )(*(pltpu.with_memory_space_constraint(v, vm) for v in results))
    return ig, gain_grad.reshape(F), bias_grad.reshape(F), wg


def solution(mesh):
    split = P(("rep", "zero"), None)
    return jax.shard_map(
        per_device,
        mesh=mesh,
        in_specs=(split, split, P(), P(), P(), split, split),
        out_specs=(split, P(), P(), P("zero", None)),
        check_vma=False,
    )
```

```python
import functools

import jax
import jax.numpy as jnp
from jax import lax
from jax.experimental import pallas as pl
from jax.experimental.pallas import tpu as pltpu
from jax.sharding import PartitionSpec as P

MESH = pl.DeviceIdType.MESH
F = 8192
ROWS = 784
CIN = 512
COUT = 2048
IMAGES = 8192
NX, NY, NZL, NZH = 4, 4, 4, 4
NZ = NZL * NZH
W = 256
F_CORE, F_X, F_Y = F // 2, F // 8, F // 32


def mul(v, m):
    return pl.multiple_of(v, m)


class Phases:
    def __init__(self):
        self.open = None

    def __call__(self, name):
        if self.open is not None:
            self.open.__exit__(None, None, None)
        self.open = None
        if name is not None:
            self.open = jax.named_scope(name)
            self.open.__enter__()


class Copies:
    def __init__(self, send, recv, partner):
        self.send, self.recv, self.partner = send, recv, partner
        self.sends, self.n_recv = [], 0

    def group(self, whole):
        self.sends.append(whole)
        return len(self.sends) - 1

    def arrivals(self, n=1):
        self.n_recv += n
        return self.n_recv - n

    def make(self, src, dst, device, group, arrival):
        return pltpu.make_async_remote_copy(
            src_ref=src,
            dst_ref=dst,
            send_sem=self.send.at[group],
            recv_sem=self.recv.at[arrival],
            device_id=device,
            device_id_type=MESH,
        )

    def start(self, *args):
        self.make(*args).start()

    def wait(self, whole, arrival):
        self.make(whole, whole, self.partner, 0, arrival).wait_recv()

    def drain(self):
        for i, whole in enumerate(self.sends):
            self.make(whole, whole, self.partner, i, 0).wait_send()


class Ring4:
    def __init__(self, copies, group, src, bufs, plus, minus):
        self.c, self.group, self.src, self.bufs = copies, group, src, bufs
        self.plus, self.minus = plus, minus
        self.arrival = copies.arrivals(3)

    def copy(self, ref, slot, device, arrival):
        self.c.start(ref, self.bufs.at[slot], device, self.group, self.arrival + arrival)

    def send2(self):
        self.copy(self.src(2, 0), 0, self.plus, 0)
        self.copy(self.src(2, 1), 1, self.minus, 1)

    def direct_plus(self):
        self.copy(self.src(1, 1), 3, self.plus, 2)

    def direct_minus(self):
        self.copy(self.src(3, 0), 2, self.minus, 2)

    def acc(self, half):
        self.c.wait(self.bufs.at[half], self.arrival + half)
        ref = self.src(1 if half == 0 else 3, half)
        ref[...] = ref[...] + self.bufs[half]
        self.copy(ref, 4 + half, self.plus if half == 0 else self.minus, 2)

    def final(self):
        self.c.wait(self.bufs.at[2:6], self.arrival + 2)
        return [self.src(0, h)[...] + self.bufs[2 + h] + self.bufs[4 + h] for h in range(2)]


def kernel(
    pre_h, up_h, gain_h, mean_h, inv_h, feat_h, og_h,
    ig, gain_o, bias_o, wg,
    pre, up, gain, mean, inv, feat, og,
    wb, wd, x1, y1, x2, y2, zs, zr,
    bnp, bnd, bnx, bnz, bna,
    local_sem, send_sem, recv_sem, know,
):
    rep, zero = lax.axis_index("rep"), lax.axis_index("zero")
    y, zl = rep // NZL, lax.rem(rep, NZL)
    core = lax.rem(zero, 2)
    xq = zero // 2
    x, zh = lax.rem(xq, NX), xq // NX
    z = zh * NZL + zl

    def at(dx=0, dy=0, dz=0, dc=0):
        zz = lax.rem(z + dz + NZ, NZ)
        xx, yy = lax.rem(x + dx + NX, NX), lax.rem(y + dy + NY, NY)
        cc = lax.rem(core + dc, 2)
        return (yy * NZL + lax.rem(zz, NZL), (zz // NZL * NX + xx) * 2 + cc)

    phase = Phases()
    phase("start")
    loads = {}

    def load(name, src, dst):
        loads[name] = pltpu.make_async_copy(src, dst, local_sem.at[len(loads)])
        loads[name].start()

    load("up", up_h, up)
    load("pre", pre_h, pre)
    load("mean", mean_h, mean)
    load("inv", inv_h, inv)
    load("feat", feat_h, feat)
    offsets = (2, 1, 3, 0)
    for k in range(4):
        for colour in range(2):
            column = mul(colour * 1024 + lax.rem(y + offsets[k], NY) * W, W)
            dst = og.at[k, :, colour * W : colour * W + W]
            load(("og", 2 * k + colour), og_h.at[:, pl.ds(column, W)], dst)
    load("gain", gain_h, gain)

    def signal(sem, device):
        pl.semaphore_signal(sem, inc=1, device_id=device, device_id_type=MESH)

    barrier = pltpu.get_barrier_semaphore()
    beside = [at(dx=1), at(dx=-1), at(dy=1), at(dy=-1)]
    near = [at(dc=1), at(dz=1), at(dz=-1)] + beside
    for device in near:
        signal(barrier, device)
    plane = [(2, 2), (2, 1), (2, 3), (1, 2), (3, 2), (1, 1), (1, 3), (3, 1), (3, 3)]
    plane += [(2, 0), (0, 2), (1, 0), (3, 0), (0, 1), (0, 3)]
    far = [8, 7, 9, 6, 10, 5, 11, 4, 12, 3, 13, 2, 14, 1, 15]

    copies = Copies(send_sem, recv_sem, at(dc=1))
    mine = core * F_CORE
    other = (1 - core) * F_CORE
    half = pl.ds(mul(mine, F_CORE), F_CORE)

    phase("bnload")
    for name in ("up", "pre", "mean", "inv"):
        loads[name].wait()

    def sums(i, carry):
        cols = pl.ds(mul(i * 512, 512), 512)
        g = up[:, cols].astype(jnp.float32)
        n = (pre[:, cols].astype(jnp.float32) - mean[:, cols]) * inv[:, cols]
        bnp[0:1, cols] = jnp.sum(g, axis=0, keepdims=True)
        bnp[1:2, cols] = jnp.sum(g * n, axis=0, keepdims=True)
        return carry

    phase("bnsum")
    lax.fori_loop(0, F // 512, sums, 0)
    phase("featwait")
    loads["feat"].wait()

    def product(k):
        loads[("og", 2 * k)].wait()
        loads[("og", 2 * k + 1)].wait()
        v = lax.dot_general(
            feat[...], og[k], (((0,), (0,)), ((), ())), preferred_element_type=jnp.float32
        )
        for c in range(2):
            for xx in range(NX):
                for zz in range(NZH):
                    dst = (xx * NZH + zz) * 16
                    src = ((zz * NX + xx) * 2 + c) * 16
                    for i in range(2):
                        wb[c, 2 * k + i, dst : dst + 16, :] = v[
                            src : src + 16, i * W : i * W + W
                        ]

    pair_group = copies.group(wd)
    pair = copies.arrivals(8)

    def pair_send(k):
        for s in (2 * k, 2 * k + 1):
            copies.start(wb.at[1 - core, s], wd.at[s], at(dc=1), pair_group, pair + s)

    phase("prod0")
    product(0)
    phase("barrier")
    pl.semaphore_wait(barrier, len(near))
    for device in beside:
        signal(know.at[3], device)
    for d in (1, -1):
        signal(know.at[0], at(dz=d))
    pair_send(0)
    bn_pair = copies.arrivals()
    copies.start(
        bnp.at[:, pl.ds(mul(other, F_CORE), F_CORE)], bnd, at(dc=1), copies.group(bnd), bn_pair
    )
    phase("prod1")
    product(1)
    pair_send(1)
    phase("prod2")
    product(2)
    pair_send(2)

    def x_rows(xx, h):
        return pl.ds(mul(lax.rem(x + xx, NX) * 64 + h * 32, 32), 32)

    order = {2: 0, 1: 1, 3: 2, 0: 3}
    x1_group, y1_group = copies.group(x1), copies.group(y1)
    ring_x1 = [
        Ring4(
            copies,
            x1_group,
            lambda off, h, k=k: wb.at[core, 2 * k, x_rows(off, h)],
            x1.at[k],
            at(dx=1),
            at(dx=-1),
        )
        for k in range(4)
    ]
    ring_y1 = [
        Ring4(
            copies,
            y1_group,
            lambda off, h, k=k: wb.at[core, 2 * order[off] + 1, x_rows(offsets[k], h)],
            y1.at[k],
            at(dy=1),
            at(dy=-1),
        )
        for k in range(4)
    ]
    ring_x2 = Ring4(
        copies,
        copies.group(x2),
        lambda off, h: wb.at[core, 2 * order[off], x_rows(0, h)],
        x2,
        at(dy=1),
        at(dy=-1),
    )
    ring_y2 = Ring4(
        copies,
        copies.group(y2),
        lambda off, h: wb.at[core, 7, x_rows(off, h)],
        y2,
        at(dx=1),
        at(dx=-1),
    )
    stage2 = (ring_x2, ring_y2)

    def pair_add(s):
        copies.wait(wd.at[s], pair + s)
        wb[core, s] = wb[core, s] + wd[s]
        if s % 2 == 0:
            ring_x1[s // 2].send2()
        elif s == 1:
            for ring in ring_y1:
                ring.send2()

    phase("add01")
    pair_add(0)
    pair_add(1)
    pl.semaphore_wait(know.at[0], 2)
    pl.semaphore_wait(know.at[3], 4)
    signal(know.at[4], at(dx=2))
    signal(know.at[4], at(dy=2))
    for d in (2, -2):
        signal(know.at[1], at(dz=d))
    phase("prod3")
    product(3)
    pair_send(3)
    phase("add23")
    pair_add(2)
    pair_add(3)
    phase("add45")
    pair_add(4)
    pair_add(5)
    phase("add67")
    pair_add(6)
    pair_add(7)

    def direct(k):
        for ring in (ring_x1[k], ring_y1[k]):
            ring.direct_plus()
            ring.direct_minus()

    def accumulate(k):
        for ring in (ring_x1[k], ring_y1[k]):
            ring.acc(0)
            ring.acc(1)

    direct(0)
    phase("bnpair")
    copies.wait(bnd, bn_pair)
    bnp[:, half] = bnp[:, half] + bnd[...]
    pl.semaphore_wait(know.at[4], 2)
    pl.semaphore_wait(know.at[1], 2)
    for d in (4, -4):
        signal(know.at[2], at(dz=d))

    def f_xy(dx, dy):
        start = mine + lax.rem(x + dx, NX) * F_X + lax.rem(y + dy, NY) * F_Y
        return pl.ds(mul(start, F_Y), F_Y)

    xy_group, xy = copies.group(bnx.at[1:16]), copies.arrivals()
    for dx, dy in plane:
        slot = bnx.at[4 * dx + dy]
        copies.start(bnp.at[:, f_xy(dx, dy)], slot, at(dx=dx, dy=dy), xy_group, xy)

    for k in range(4):
        phase(f"acc{k}")
        accumulate(k)
        if k < 3:
            direct(k + 1)

    phase("bnxy")
    copies.wait(bnx.at[1:16], xy)
    pl.semaphore_wait(know.at[2], 2)
    total = bnp[:, f_xy(0, 0)]
    for dx, dy in plane:
        total = total + bnx[4 * dx + dy]
    bnz[z] = total
    bz_group, bz = copies.group(bnz.at[0:15]), copies.arrivals()
    for d in far:
        copies.start(bnz.at[z], bnz.at[z], at(dz=d), bz_group, bz)

    def final(k):
        for h, v in enumerate(ring_x1[k].final()):
            wb[core, 2 * k, x_rows(0, h)] = v
        for h, v in enumerate(ring_y1[k].final()):
            wb[core, 7, x_rows(offsets[k], h)] = v

    phase("fin0")
    final(0)
    for ring in stage2:
        ring.send2()
    phase("fin1")
    final(1)
    for ring in stage2:
        ring.direct_plus()
    phase("fin2")
    final(2)
    for ring in stage2:
        ring.direct_minus()
    phase("accs2")
    for ring in stage2:
        ring.acc(0)
        ring.acc(1)
    phase("fin3")
    final(3)

    z_group, z_arrival = copies.group(zr.at[0:15]), copies.arrivals()

    def weight_z(colour):
        for h, v in enumerate(stage2[colour].final()):
            for i in range(2):
                zs[2 * colour + i, h * 32 : h * 32 + 32, :] = v[:, i * 128 : i * 128 + 128]
        for j in range(8):
            ll, hh = 2 * colour + j % 2, lax.rem(zh + offsets[j // 2], NZH)
            copy = copies.make(
                zs.at[ll, pl.ds(mul(hh * 16, 16), 16)],
                zr.at[z],
                (y * NZL + ll, (hh * NX + x) * 2 + core),
                z_group,
                z_arrival,
            )
            if j < 6:
                copy.start()
            else:
                pl.when(ll != zl)(copy.start)

    phase("wgtz0")
    weight_z(0)
    phase("wgtz1")
    weight_z(1)

    phase("bnz")
    copies.wait(bnz.at[0:15], bz)
    total = bnz[0]
    for i in range(1, NZ):
        total = total + bnz[i]
    own = bna.at[:, f_xy(0, 0)]
    own[...] = total * (1.0 / IMAGES)
    axy_group, axy = copies.group(bnz.at[0:15]), copies.arrivals()
    for dx, dy in plane:
        copies.start(own, own, at(dx=dx, dy=dy), axy_group, axy)
    zr[z] = zs[zl, pl.ds(mul(zh * 16, 16), 16)]

    phase("zwait")
    copies.wait(zr.at[0:15], z_arrival)
    result = zr[0]
    for i in range(1, NZ):
        result = result + zr[i]
    column = mul(zl // 2 * 1024 + y * W + lax.rem(zl, 2) * 128, 128)
    piece = wg.at[:, pl.ds(column, 128)]
    piece[...] = result * (1.0 / IMAGES)

    phase("ag")
    peers = [(2, 3), (2, 1), (2, 2), (1, 3), (3, 3), (1, 1), (3, 1), (1, 2), (3, 2)]
    peers += [(2, 0), (0, 3), (0, 1), (0, 2), (1, 0), (3, 0)]
    ag_group, ag = copies.group(zr.at[0:15]), copies.arrivals()
    for dy, dl in peers:
        device = (lax.rem(y + dy, NY) * NZL + lax.rem(zl + dl, NZL), zero)
        copies.start(piece, piece, device, ag_group, ag)

    phase("bngxy")
    copies.wait(bnz.at[0:15], axy)
    ap = copies.arrivals()
    whole_half = bna.at[:, half]
    copies.start(whole_half, whole_half, at(dc=1), copies.group(bnd), ap)
    phase("bngp")
    copies.wait(bnd, ap)
    loads["gain"].wait()

    def grads(i, carry):
        cols = pl.ds(mul(i * 512, 512), 512)
        g = up[:, cols].astype(jnp.float32)
        n = (pre[:, cols].astype(jnp.float32) - mean[:, cols]) * inv[:, cols]
        scale = gain[:, cols] * inv[:, cols]
        bias_grad, gain_grad = bna[0:1, cols], bna[1:2, cols]
        bias_o[:, cols] = bias_grad
        gain_o[:, cols] = gain_grad
        ig[:, cols] = (scale * (g - bias_grad - n * gain_grad)).astype(jnp.bfloat16)
        return carry

    phase("grads")
    lax.fori_loop(0, F // 512, grads, 0)
    phase("agwait")
    copies.wait(zr.at[0:15], ag)
    phase("drain")
    copies.drain()
    phase(None)
    assert (len(copies.sends), copies.n_recv) == (N_SEND, N_RECV), "semaphore counts"


N_SEND, N_RECV = 12, 45


def store(ig, gain, bias, wg, ig_o, gain_o, bias_o, wg_o, sem):
    pairs = ((ig, ig_o), (wg, wg_o), (gain, gain_o), (bias, bias_o))
    copies = [pltpu.make_async_copy(a, b, sem.at[i]) for i, (a, b) in enumerate(pairs)]
    for copy in copies:
        copy.start()
    for copy in copies:
        copy.wait()


def per_device(pre_norm, upstream, norm_gain, saved_mean, inv_std, features, out_grads):
    row = lambda v: v.reshape(1, F)
    f32, bf16 = jnp.float32, jnp.bfloat16
    vm = pltpu.VMEM
    dma = pltpu.SemaphoreType.DMA
    outs = (
        jax.ShapeDtypeStruct((16, F), bf16),
        jax.ShapeDtypeStruct((1, F), f32),
        jax.ShapeDtypeStruct((1, F), f32),
        jax.ShapeDtypeStruct((16, COUT), f32),
    )
    vectors = (row(norm_gain), row(saved_mean), row(inv_std))
    arrays = (pre_norm, upstream, *vectors, features, out_grads)
    results = pl.pallas_call(
        kernel,
        out_shape=outs,
        in_specs=[pl.BlockSpec(memory_space=pltpu.HBM)] * 7,
        out_specs=(pl.BlockSpec(memory_space=vm),) * 4,
        scratch_shapes=[
            vm((16, F), bf16), vm((16, F), bf16), vm((1, F), f32), vm((1, F), f32), vm((1, F), f32),
            vm((ROWS, CIN), bf16), vm((4, ROWS, 2 * W), bf16),
            vm((2, 8, 256, W), f32), vm((8, 256, W), f32),
            vm((4, 6, 32, W), f32), vm((4, 6, 32, W), f32), vm((6, 32, W), f32), vm((6, 32, W), f32),
            vm((NZL, 64, 128), f32), vm((NZ, 16, 128), f32),
            vm((2, F), f32), vm((2, F_CORE), f32), vm((16, 2, F_Y), f32),
            vm((NZ, 2, F_Y), f32), vm((2, F), f32),
            dma((14,)), dma((N_SEND,)), dma((N_RECV,)), pltpu.SemaphoreType.REGULAR((5,)),
        ],
        compiler_params=pltpu.CompilerParams(
            collective_id=0, has_side_effects=True, vmem_limit_bytes=32 * 1024 * 1024
        ),
        name="twins",
    )(*(pltpu.with_memory_space_constraint(v, pltpu.HBM) for v in arrays))
    ig, gain_grad, bias_grad, wg = pl.pallas_call(
        store,
        out_shape=outs,
        in_specs=[pl.BlockSpec(memory_space=pl.ANY)] * 4,
        out_specs=(pl.BlockSpec(memory_space=pltpu.HBM),) * 4,
        scratch_shapes=[dma((4,))],
        name="store",
    )(*(pltpu.with_memory_space_constraint(v, vm) for v in results))
    return ig, gain_grad.reshape(F), bias_grad.reshape(F), wg


def solution(mesh):
    split = P(("rep", "zero"), None)
    return jax.shard_map(
        per_device,
        mesh=mesh,
        in_specs=(split, split, P(), P(), P(), split, split),
        out_specs=(split, P(), P(), P("zero", None)),
        check_vma=False,
    )
```

```python
import functools

import jax
import jax.numpy as jnp
from jax import lax
from jax.experimental import pallas as pl
from jax.experimental.pallas import tpu as pltpu
from jax.sharding import PartitionSpec as P

MESH = pl.DeviceIdType.MESH
F = 8192
ROWS = 784
CIN = 512
COUT = 2048
IMAGES = 8192
NX, NY, NZL, NZH = 4, 4, 4, 4
NZ = NZL * NZH
W = 256
F_CORE, F_X, F_Y = F // 2, F // 8, F // 32


def mul(v, m):
    return pl.multiple_of(v, m)


class Phases:
    def __init__(self):
        self.open = None

    def __call__(self, name):
        if self.open is not None:
            self.open.__exit__(None, None, None)
        self.open = None
        if name is not None:
            self.open = jax.named_scope(name)
            self.open.__enter__()


class Copies:
    def __init__(self, send, recv, partner):
        self.send, self.recv, self.partner = send, recv, partner
        self.sends, self.n_recv = [], 0

    def group(self, whole):
        self.sends.append(whole)
        return len(self.sends) - 1

    def arrivals(self, n=1):
        self.n_recv += n
        return self.n_recv - n

    def make(self, src, dst, device, group, arrival):
        return pltpu.make_async_remote_copy(
            src_ref=src,
            dst_ref=dst,
            send_sem=self.send.at[group],
            recv_sem=self.recv.at[arrival],
            device_id=device,
            device_id_type=MESH,
        )

    def start(self, *args):
        self.make(*args).start()

    def wait(self, whole, arrival):
        self.make(whole, whole, self.partner, 0, arrival).wait_recv()

    def drain(self):
        for i, whole in enumerate(self.sends):
            self.make(whole, whole, self.partner, i, 0).wait_send()


class Ring4:
    def __init__(self, copies, group, src, bufs, plus, minus, split=False):
        self.c, self.group, self.src, self.bufs = copies, group, src, bufs
        self.plus, self.minus = plus, minus
        self.arrival = copies.arrivals(3 if split else 2)
        self.split = split

    def copy(self, ref, slot, device, arrival):
        self.c.start(ref, self.bufs.at[slot], device, self.group, self.arrival + arrival)

    def send2(self):
        self.copy(self.src(2, 0), 0, self.plus, 1)
        self.copy(self.src(2, 1), 1, self.minus, 2 if self.split else 1)

    def direct_plus(self):
        self.copy(self.src(1, 1), 3, self.plus, 0)

    def direct_minus(self):
        self.copy(self.src(3, 0), 2, self.minus, 0)

    def acc(self, half):
        if self.split:
            self.c.wait(self.bufs.at[half], self.arrival + 1 + half)
        elif half == 0:
            self.c.wait(self.bufs.at[0:2], self.arrival + 1)
        ref = self.src(1 if half == 0 else 3, half)
        ref[...] = ref[...] + self.bufs[half]
        self.copy(ref, 4 + half, self.plus if half == 0 else self.minus, 0)

    def final(self):
        self.c.wait(self.bufs.at[2:6], self.arrival)
        return [self.src(0, h)[...] + self.bufs[2 + h] + self.bufs[4 + h] for h in range(2)]


def kernel(
    pre_h, up_h, gain_h, mean_h, inv_h, feat_h, og_h,
    ig, gain_o, bias_o, wg,
    rows, vectors, feat, og,
    wb, wd, rings, zs, zr,
    bnp, bnd, bnx, bnz, bna,
    local_sem, send_sem, recv_sem, know,
):
    rep, zero = lax.axis_index("rep"), lax.axis_index("zero")
    y, zl = rep // NZL, lax.rem(rep, NZL)
    core = lax.rem(zero, 2)
    xq = zero // 2
    x, zh = lax.rem(xq, NX), xq // NX
    z = zh * NZL + zl

    def at(dx=0, dy=0, dz=0, dc=0):
        zz = lax.rem(z + dz + NZ, NZ)
        xx, yy = lax.rem(x + dx + NX, NX), lax.rem(y + dy + NY, NY)
        cc = lax.rem(core + dc, 2)
        return (yy * NZL + lax.rem(zz, NZL), (zz // NZL * NX + xx) * 2 + cc)

    phase = Phases()
    phase("start")
    offsets = (2, 1, 3, 0)
    pltpu.make_async_copy(feat_h, feat, local_sem.at[4]).start()
    for k in range(4):
        for colour in range(2):
            column = mul(colour * 1024 + lax.rem(y + offsets[k], NY) * W, W)
            dst = og.at[k, :, colour * W : colour * W + W]
            pltpu.make_async_copy(og_h.at[:, pl.ds(column, W)], dst, local_sem.at[k]).start()
        if k == 1:
            pltpu.make_async_copy(up_h, rows.at[0], local_sem.at[5]).start()
            pltpu.make_async_copy(pre_h, rows.at[1], local_sem.at[5]).start()
            for i, v in enumerate((mean_h, inv_h, gain_h)):
                pltpu.make_async_copy(v, vectors.at[i], local_sem.at[6]).start()

    def loaded(ref, i):
        pltpu.make_async_remote_copy(
            src_ref=ref,
            dst_ref=ref,
            send_sem=local_sem.at[i],
            recv_sem=local_sem.at[i],
            device_id=at(dc=1),
            device_id_type=MESH,
        ).wait_recv()

    up, pre = rows.at[0], rows.at[1]
    mean, inv, gain = vectors.at[0], vectors.at[1], vectors.at[2]

    def signal(sem, device):
        pl.semaphore_signal(sem, inc=1, device_id=device, device_id_type=MESH)

    barrier = pltpu.get_barrier_semaphore()
    beside = [at(dx=1), at(dx=-1), at(dy=1), at(dy=-1)]
    near = [at(dc=1), at(dz=1), at(dz=-1)] + beside
    for device in near:
        signal(barrier, device)
    plane = [(2, 2), (2, 1), (2, 3), (1, 2), (3, 2), (1, 1), (1, 3), (3, 1), (3, 3)]
    plane += [(2, 0), (0, 2), (1, 0), (3, 0), (0, 1), (0, 3)]
    far = [8, 7, 9, 6, 10, 5, 11, 4, 12, 3, 13, 2, 14, 1, 15]

    copies = Copies(send_sem, recv_sem, at(dc=1))
    mine = core * F_CORE
    other = (1 - core) * F_CORE
    half = pl.ds(mul(mine, F_CORE), F_CORE)

    phase("featwait")
    loaded(feat, 4)

    def product(k):
        loaded(og.at[k], k)
        v = lax.dot_general(
            feat[...], og[k], (((0,), (0,)), ((), ())), preferred_element_type=jnp.float32
        )
        for c in range(2):
            for xx in range(NX):
                for zz in range(NZH):
                    dst = (xx * NZH + zz) * 16
                    src = ((zz * NX + xx) * 2 + c) * 16
                    for i in range(2):
                        wb[c, 2 * k + i, dst : dst + 16, :] = v[
                            src : src + 16, i * W : i * W + W
                        ]

    pair_group = copies.group(wd)
    pair = copies.arrivals(8)

    def pair_send(k):
        for s in (2 * k, 2 * k + 1):
            copies.start(wb.at[1 - core, s], wd.at[s], at(dc=1), pair_group, pair + s)

    phase("prod0")
    product(0)
    phase("barrier")
    pl.semaphore_wait(barrier, len(near))
    for device in beside:
        signal(know.at[3], device)
    for d in (1, -1):
        signal(know.at[0], at(dz=d))
    pair_send(0)
    phase("prod1")
    product(1)
    pair_send(1)
    phase("bnload")
    loaded(rows, 5)
    loaded(vectors, 6)

    def sums(i, carry):
        cols = pl.ds(mul(i * 512, 512), 512)
        g = up[:, cols].astype(jnp.float32)
        n = (pre[:, cols].astype(jnp.float32) - mean[:, cols]) * inv[:, cols]
        bnp[0:1, cols] = jnp.sum(g, axis=0, keepdims=True)
        bnp[1:2, cols] = jnp.sum(g * n, axis=0, keepdims=True)
        return carry

    phase("bnsum")
    lax.fori_loop(0, F // 512, sums, 0)
    bn_pair = copies.arrivals()
    copies.start(
        bnp.at[:, pl.ds(mul(other, F_CORE), F_CORE)], bnd, at(dc=1), copies.group(bnd), bn_pair
    )
    def x_rows(xx, h):
        return pl.ds(mul(lax.rem(x + xx, NX) * 64 + h * 32, 32), 32)

    order = {2: 0, 1: 1, 3: 2, 0: 3}
    ring_group = copies.group(rings)
    ring_x1 = [
        Ring4(
            copies,
            ring_group,
            lambda off, h, k=k: wb.at[core, 2 * k, x_rows(off, h)],
            rings.at[k],
            at(dx=1),
            at(dx=-1),
        )
        for k in range(4)
    ]
    ring_y1 = [
        Ring4(
            copies,
            ring_group,
            lambda off, h, k=k: wb.at[core, 2 * order[off] + 1, x_rows(offsets[k], h)],
            rings.at[4 + k],
            at(dy=1),
            at(dy=-1),
        )
        for k in range(4)
    ]
    ring_x2 = Ring4(
        copies,
        ring_group,
        lambda off, h: wb.at[core, 2 * order[off], x_rows(0, h)],
        rings.at[8],
        at(dy=1),
        at(dy=-1),
        split=True,
    )
    ring_y2 = Ring4(
        copies,
        ring_group,
        lambda off, h: wb.at[core, 7, x_rows(off, h)],
        rings.at[9],
        at(dx=1),
        at(dx=-1),
        split=True,
    )
    stage2 = (ring_x2, ring_y2)

    def pair_add(s):
        copies.wait(wd.at[s], pair + s)
        wb[core, s] = wb[core, s] + wd[s]

    def direct(ring):
        ring.direct_plus()
        ring.direct_minus()

    def accumulate(ring):
        ring.acc(0)
        ring.acc(1)

    def final_x(k):
        for h, v in enumerate(ring_x1[k].final()):
            wb[core, 2 * k, x_rows(0, h)] = v

    def final_y(k):
        for h, v in enumerate(ring_y1[k].final()):
            wb[core, 7, x_rows(offsets[k], h)] = v

    phase("add0")
    pair_add(0)
    ring_x1[0].send2()
    direct(ring_x1[0])
    pl.semaphore_wait(know.at[0], 2)
    pl.semaphore_wait(know.at[3], 4)
    signal(know.at[4], at(dx=2))
    signal(know.at[4], at(dy=2))
    for d in (2, -2):
        signal(know.at[1], at(dz=d))
    phase("prod2")
    product(2)
    pair_send(2)
    phase("add12")
    pair_add(1)
    ring_y1[0].send2()
    ring_y1[1].send2()
    pair_add(2)
    ring_x1[1].send2()
    phase("prod3")
    product(3)
    pair_send(3)
    phase("add3")
    pair_add(3)
    ring_y1[2].send2()
    ring_y1[3].send2()
    ring_y1[0].direct_plus()
    phase("bnpair")
    copies.wait(bnd, bn_pair)
    bnp[:, half] = bnp[:, half] + bnd[...]
    pl.semaphore_wait(know.at[4], 2)
    pl.semaphore_wait(know.at[1], 2)
    for d in (4, -4):
        signal(know.at[2], at(dz=d))

    def f_xy(dx, dy):
        start = mine + lax.rem(x + dx, NX) * F_X + lax.rem(y + dy, NY) * F_Y
        return pl.ds(mul(start, F_Y), F_Y)

    xy_group, xy = copies.group(bnx.at[1:16]), copies.arrivals()
    for dx, dy in plane:
        slot = bnx.at[4 * dx + dy]
        copies.start(bnp.at[:, f_xy(dx, dy)], slot, at(dx=dx, dy=dy), xy_group, xy)

    phase("add45")
    pair_add(4)
    ring_x1[2].send2()
    pair_add(5)
    ring_y1[0].direct_minus()
    phase("acc0")
    accumulate(ring_x1[0])
    phase("add67")
    pair_add(6)
    ring_x1[3].send2()
    direct(ring_x1[1])
    pair_add(7)
    phase("acc0y")
    accumulate(ring_y1[0])
    direct(ring_y1[1])
    def bn_z():
        copies.wait(bnx.at[1:16], xy)
        pl.semaphore_wait(know.at[2], 2)
        total = bnp[:, f_xy(0, 0)]
        for dx, dy in plane:
            total = total + bnx[4 * dx + dy]
        bnz[z] = total
        bz_group, bz = copies.group(bnz.at[0:15]), copies.arrivals()
        for d in far:
            copies.start(bnz.at[z], bnz.at[z], at(dz=d), bz_group, bz)
        return bz

    first, second = {"X": ring_x1, "Y": ring_y1}, {"X": ring_x2, "Y": ring_y2}
    finals = {"X": final_x, "Y": final_y}

    bz = None
    for step in " ".join(ORDER).split():
        phase(step)
        kind, c, k = step[0], step[1:2], int(step[2:3] or 0)
        if kind == "a":
            accumulate(first[c][k])
        elif kind == "d":
            direct(first[c][k])
        elif kind == "s":
            second[c].acc(k)
        elif kind == "f":
            finals[c](k)
            if k < 3:
                (second[c].send2, second[c].direct_plus, second[c].direct_minus)[k]()
        else:
            bz = bn_z()

    z_group, z_arrival = copies.group(zr.at[0:15]), copies.arrivals()

    def weight_z(colour):
        for h, v in enumerate(stage2[colour].final()):
            for i in range(2):
                zs[2 * colour + i, h * 32 : h * 32 + 32, :] = v[:, i * 128 : i * 128 + 128]
        for j in range(8):
            ll, hh = 2 * colour + j % 2, lax.rem(zh + offsets[j // 2], NZH)
            copy = copies.make(
                zs.at[ll, pl.ds(mul(hh * 16, 16), 16)],
                zr.at[z],
                (y * NZL + ll, (hh * NX + x) * 2 + core),
                z_group,
                z_arrival,
            )
            if j < 6:
                copy.start()
            else:
                pl.when(ll != zl)(copy.start)

    phase("wgtz0")
    weight_z(0)
    phase("wgtz1")
    weight_z(1)

    phase("bnz")
    copies.wait(bnz.at[0:15], bz)
    total = bnz[0]
    for i in range(1, NZ):
        total = total + bnz[i]
    own = bna.at[:, f_xy(0, 0)]
    own[...] = total * (1.0 / IMAGES)
    others = bna.at[:, 0 : 31 * F_Y]
    axy_group, axy = copies.group(others), copies.arrivals()
    for dx, dy in plane + [(0, 0)]:
        for dc in (1, 0):
            if dx or dy or dc:
                copies.start(own, own, at(dx=dx, dy=dy, dc=dc), axy_group, axy)
    zr[z] = zs[zl, pl.ds(mul(zh * 16, 16), 16)]

    phase("zwait")
    copies.wait(zr.at[0:15], z_arrival)
    result = zr[0]
    for i in range(1, NZ):
        result = result + zr[i]
    column = mul(zl // 2 * 1024 + y * W + lax.rem(zl, 2) * 128, 128)
    piece = wg.at[:, pl.ds(column, 128)]
    piece[...] = result * (1.0 / IMAGES)

    phase("ag")
    peers = [(2, 3), (2, 1), (2, 2), (1, 3), (3, 3), (1, 1), (3, 1), (1, 2), (3, 2)]
    peers += [(2, 0), (0, 3), (0, 1), (0, 2), (1, 0), (3, 0)]
    ag_group, ag = copies.group(zr.at[0:15]), copies.arrivals()
    for dy, dl in peers:
        device = (lax.rem(y + dy, NY) * NZL + lax.rem(zl + dl, NZL), zero)
        copies.start(piece, piece, device, ag_group, ag)

    phase("bngxy")
    copies.wait(others, axy)

    def grads(i, carry):
        cols = pl.ds(mul(i * 512, 512), 512)
        g = up[:, cols].astype(jnp.float32)
        n = (pre[:, cols].astype(jnp.float32) - mean[:, cols]) * inv[:, cols]
        scale = gain[:, cols] * inv[:, cols]
        bias_grad, gain_grad = bna[0:1, cols], bna[1:2, cols]
        bias_o[:, cols] = bias_grad
        gain_o[:, cols] = gain_grad
        ig[:, cols] = (scale * (g - bias_grad - n * gain_grad)).astype(jnp.bfloat16)
        return carry

    phase("grads")
    lax.fori_loop(0, F // 512, grads, 0)
    phase("agwait")
    copies.wait(zr.at[0:15], ag)
    phase("drain")
    copies.drain()
    phase(None)
    assert (len(copies.sends), copies.n_recv) == (N_SEND, N_RECV), "semaphore counts"


N_SEND, N_RECV = 8, 36
ORDER = (
    "aX1 dX2 aY1 aX2", "fX0 dY2 aY2 dX3", "fY0 fX1 dY3 aX3", "aY3 fY1 b",
    "sX0 sY0 fX2 sX1", "fY2 sY1 fX3 fY3",
)


def store(ig, gain, bias, wg, ig_o, gain_o, bias_o, wg_o, sem):
    pairs = ((ig, ig_o), (wg, wg_o), (gain, gain_o), (bias, bias_o))
    copies = [pltpu.make_async_copy(a, b, sem.at[i]) for i, (a, b) in enumerate(pairs)]
    for copy in copies:
        copy.start()
    for copy in copies:
        copy.wait()


def per_device(pre_norm, upstream, norm_gain, saved_mean, inv_std, features, out_grads):
    row = lambda v: v.reshape(1, F)
    f32, bf16 = jnp.float32, jnp.bfloat16
    vm = pltpu.VMEM
    dma = pltpu.SemaphoreType.DMA
    outs = (
        jax.ShapeDtypeStruct((16, F), bf16),
        jax.ShapeDtypeStruct((1, F), f32),
        jax.ShapeDtypeStruct((1, F), f32),
        jax.ShapeDtypeStruct((16, COUT), f32),
    )
    vectors = (row(norm_gain), row(saved_mean), row(inv_std))
    arrays = (pre_norm, upstream, *vectors, features, out_grads)
    results = pl.pallas_call(
        kernel,
        out_shape=outs,
        in_specs=[pl.BlockSpec(memory_space=pltpu.HBM)] * 7,
        out_specs=(pl.BlockSpec(memory_space=vm),) * 4,
        scratch_shapes=[
            vm((2, 16, F), bf16), vm((3, 1, F), f32), vm((ROWS, CIN), bf16), vm((4, ROWS, 2 * W), bf16),
            vm((2, 8, 256, W), f32), vm((8, 256, W), f32),
            vm((10, 6, 32, W), f32),
            vm((NZL, 64, 128), f32), vm((NZ, 16, 128), f32),
            vm((2, F), f32), vm((2, F_CORE), f32), vm((16, 2, F_Y), f32),
            vm((NZ, 2, F_Y), f32), vm((2, F), f32),
            dma((7,)), dma((N_SEND,)), dma((N_RECV,)), pltpu.SemaphoreType.REGULAR((5,)),
        ],
        compiler_params=pltpu.CompilerParams(
            collective_id=0, has_side_effects=True, vmem_limit_bytes=32 * 1024 * 1024
        ),
        name="twins",
    )(*(pltpu.with_memory_space_constraint(v, pltpu.HBM) for v in arrays))
    ig, gain_grad, bias_grad, wg = pl.pallas_call(
        store,
        out_shape=outs,
        in_specs=[pl.BlockSpec(memory_space=pl.ANY)] * 4,
        out_specs=(pl.BlockSpec(memory_space=pltpu.HBM),) * 4,
        scratch_shapes=[dma((4,))],
        name="store",
    )(*(pltpu.with_memory_space_constraint(v, vm) for v in results))
    return ig, gain_grad.reshape(F), bias_grad.reshape(F), wg


def solution(mesh):
    split = P(("rep", "zero"), None)
    return jax.shard_map(
        per_device,
        mesh=mesh,
        in_specs=(split, split, P(), P(), P(), split, split),
        out_specs=(split, P(), P(), P("zero", None)),
        check_vma=False,
    )
```

```python
import functools

import jax
import jax.numpy as jnp
from jax import lax
from jax.experimental import pallas as pl
from jax.experimental.pallas import tpu as pltpu
from jax.sharding import PartitionSpec as P

MESH = pl.DeviceIdType.MESH
F = 8192
ROWS = 784
CIN = 512
COUT = 2048
IMAGES = 8192
NX, NY, NZL, NZH = 4, 4, 4, 4
NZ = NZL * NZH
W = 256
F_CORE, F_X, F_Y = F // 2, F // 8, F // 32


def mul(v, m):
    return pl.multiple_of(v, m)


class Phases:
    def __init__(self):
        self.open = None

    def __call__(self, name):
        if self.open is not None:
            self.open.__exit__(None, None, None)
        self.open = None
        if name is not None:
            self.open = jax.named_scope(name)
            self.open.__enter__()


class Copies:
    def __init__(self, send, recv, partner):
        self.send, self.recv, self.partner = send, recv, partner
        self.sends, self.n_recv = [], 0

    def group(self, whole):
        self.sends.append(whole)
        return len(self.sends) - 1

    def arrivals(self, n=1):
        self.n_recv += n
        return self.n_recv - n

    def make(self, src, dst, device, group, arrival):
        return pltpu.make_async_remote_copy(
            src_ref=src,
            dst_ref=dst,
            send_sem=self.send.at[group],
            recv_sem=self.recv.at[arrival],
            device_id=device,
            device_id_type=MESH,
        )

    def start(self, *args):
        self.make(*args).start()

    def wait(self, whole, arrival):
        self.make(whole, whole, self.partner, 0, arrival).wait_recv()

    def drain(self):
        for i, whole in enumerate(self.sends):
            self.make(whole, whole, self.partner, i, 0).wait_send()


class Ring4:
    def __init__(self, copies, group, src, bufs, plus, minus, split=False):
        self.c, self.group, self.src, self.bufs = copies, group, src, bufs
        self.plus, self.minus = plus, minus
        self.arrival = copies.arrivals(3 if split else 2)
        self.split = split

    def copy(self, ref, slot, device, arrival):
        self.c.start(ref, self.bufs.at[slot], device, self.group, self.arrival + arrival)

    def send2(self):
        self.copy(self.src(2, 0), 0, self.plus, 1)
        self.copy(self.src(2, 1), 1, self.minus, 2 if self.split else 1)

    def direct_plus(self):
        self.copy(self.src(1, 1), 3, self.plus, 0)

    def direct_minus(self):
        self.copy(self.src(3, 0), 2, self.minus, 0)

    def acc(self, half):
        if self.split:
            self.c.wait(self.bufs.at[half], self.arrival + 1 + half)
        elif half == 0:
            self.c.wait(self.bufs.at[0:2], self.arrival + 1)
        ref = self.src(1 if half == 0 else 3, half)
        ref[...] = ref[...] + self.bufs[half]
        self.copy(ref, 4 + half, self.plus if half == 0 else self.minus, 0)

    def final(self):
        self.c.wait(self.bufs.at[2:6], self.arrival)
        return [self.src(0, h)[...] + self.bufs[2 + h] + self.bufs[4 + h] for h in range(2)]


def kernel(
    pre_h, up_h, gain_h, mean_h, inv_h, feat_h, og_h,
    ig, gain_o, bias_o, wg,
    rows, vectors, feat, og,
    wb, wd, rings, half_rings, zx, zy, own_sums, zs, zr,
    bnp, bnd, bnx, bnz, bna,
    local_sem, send_sem, recv_sem, know,
):
    rep, zero = lax.axis_index("rep"), lax.axis_index("zero")
    y, zl = rep // NZL, lax.rem(rep, NZL)
    core = lax.rem(zero, 2)
    xq = zero // 2
    x, zh = lax.rem(xq, NX), xq // NX
    z = zh * NZL + zl

    def at(dx=0, dy=0, dz=0, dc=0):
        zz = lax.rem(z + dz + NZ, NZ)
        xx, yy = lax.rem(x + dx + NX, NX), lax.rem(y + dy + NY, NY)
        cc = lax.rem(core + dc, 2)
        return (yy * NZL + lax.rem(zz, NZL), (zz // NZL * NX + xx) * 2 + cc)

    phase = Phases()
    phase("start")
    offsets, own_early = (2, 1, 3, 0), (2, 1, 0, 3)
    slot_x = (0, 2, 6, 4)
    pltpu.make_async_copy(feat_h, feat, local_sem.at[4]).start()
    for k in range(4):
        for colour in range(2):
            off = (offsets, own_early)[colour == 0][k]
            column = mul(colour * 1024 + lax.rem(y + off, NY) * W, W)
            dst = og.at[k, :, colour * W : colour * W + W]
            pltpu.make_async_copy(og_h.at[:, pl.ds(column, W)], dst, local_sem.at[k]).start()
        if k == 1:
            pltpu.make_async_copy(up_h, rows.at[0], local_sem.at[5]).start()
            pltpu.make_async_copy(pre_h, rows.at[1], local_sem.at[5]).start()
            for i, v in enumerate((mean_h, inv_h, gain_h)):
                pltpu.make_async_copy(v, vectors.at[i], local_sem.at[6]).start()

    def loaded(ref, i):
        pltpu.make_async_remote_copy(
            src_ref=ref,
            dst_ref=ref,
            send_sem=local_sem.at[i],
            recv_sem=local_sem.at[i],
            device_id=at(dc=1),
            device_id_type=MESH,
        ).wait_recv()

    up, pre = rows.at[0], rows.at[1]
    mean, inv, gain = vectors.at[0], vectors.at[1], vectors.at[2]

    def signal(sem, device):
        pl.semaphore_signal(sem, inc=1, device_id=device, device_id_type=MESH)

    barrier = pltpu.get_barrier_semaphore()
    beside = [at(dx=1), at(dx=-1), at(dy=1), at(dy=-1)]
    near = [at(dc=1), at(dz=1), at(dz=-1)] + beside
    for device in near:
        signal(barrier, device)
    plane = [(2, 2), (2, 1), (2, 3), (1, 2), (3, 2), (1, 1), (1, 3), (3, 1), (3, 3)]
    plane += [(2, 0), (0, 2), (1, 0), (3, 0), (0, 1), (0, 3)]
    far = [8, 7, 9, 6, 10, 5, 11, 4, 12, 3, 13, 2, 14, 1, 15]

    copies = Copies(send_sem, recv_sem, at(dc=1))
    mine = core * F_CORE
    other = (1 - core) * F_CORE
    half = pl.ds(mul(mine, F_CORE), F_CORE)

    phase("featwait")
    loaded(feat, 4)

    def product(k):
        loaded(og.at[k], k)
        v = lax.dot_general(
            feat[...], og[k], (((0,), (0,)), ((), ())), preferred_element_type=jnp.float32
        )
        for c in range(2):
            for xx in range(NX):
                for zz in range(NZH):
                    dst = (xx * NZH + zz) * 16
                    src = ((zz * NX + xx) * 2 + c) * 16
                    for i in range(2):
                        wb[c, 2 * k + i, dst : dst + 16, :] = v[
                            src : src + 16, i * W : i * W + W
                        ]

    pair_group = copies.group(wd)
    pair = copies.arrivals(8)

    def pair_send(k):
        for s in (2 * k, 2 * k + 1):
            copies.start(wb.at[1 - core, s], wd.at[s], at(dc=1), pair_group, pair + s)

    phase("prod0")
    product(0)
    phase("barrier")
    pl.semaphore_wait(barrier, len(near))
    for device in beside:
        signal(know.at[3], device)
    for d in (1, -1):
        signal(know.at[0], at(dz=d))
    pair_send(0)
    phase("prod1")
    product(1)
    pair_send(1)
    phase("bnload")
    loaded(rows, 5)
    loaded(vectors, 6)

    def sums(i, carry):
        cols = pl.ds(mul(i * 512, 512), 512)
        g = up[:, cols].astype(jnp.float32)
        n = (pre[:, cols].astype(jnp.float32) - mean[:, cols]) * inv[:, cols]
        bnp[0:1, cols] = jnp.sum(g, axis=0, keepdims=True)
        bnp[1:2, cols] = jnp.sum(g * n, axis=0, keepdims=True)
        return carry

    phase("bnsum")
    lax.fori_loop(0, F // 512, sums, 0)
    bn_pair = copies.arrivals()
    copies.start(
        bnp.at[:, pl.ds(mul(other, F_CORE), F_CORE)], bnd, at(dc=1), copies.group(bnd), bn_pair
    )
    def x_rows(xx, h):
        return pl.ds(mul(lax.rem(x + xx, NX) * 64 + h * 32, 32), 32)

    order = {2: 0, 1: 1, 3: 2, 0: 3}
    ring_group, half_group = copies.group(rings), copies.group(half_rings)
    parity = lax.rem(zl, 2)
    kept = pl.ds(mul(parity * 128, 128), 128)
    given = pl.ds(mul((1 - parity) * 128, 128), 128)

    def bufs(k, colour):
        return half_rings.at[colour] if k == 3 else rings.at[3 * colour + k]

    def columns(k):
        return kept if k == 3 else slice(None)

    ring_x1 = [
        Ring4(
            copies,
            half_group if k == 3 else ring_group,
            lambda off, h, k=k: wb.at[core, slot_x[k], x_rows(off, h), columns(k)],
            bufs(k, 0),
            at(dx=1),
            at(dx=-1),
        )
        for k in range(4)
    ]
    ring_y1 = [
        Ring4(
            copies,
            half_group if k == 3 else ring_group,
            lambda off, h, k=k: wb.at[
                core, 2 * order[off] + 1, x_rows(offsets[k], h), columns(k)
            ],
            bufs(k, 1),
            at(dy=1),
            at(dy=-1),
        )
        for k in range(4)
    ]
    ring_x2 = Ring4(
        copies,
        ring_group,
        lambda off, h: (
            wb.at[core, slot_x[order[off]], x_rows(0, h)] if off else own_sums.at[0, h]
        ),
        rings.at[6],
        at(dy=1),
        at(dy=-1),
        split=True,
    )
    ring_y2 = Ring4(
        copies,
        ring_group,
        lambda off, h: wb.at[core, 7, x_rows(off, h)] if off else own_sums.at[1, h],
        rings.at[7],
        at(dx=1),
        at(dx=-1),
        split=True,
    )
    zx_group, zy_group = copies.group(zx), copies.group(zy)
    zx_arrival, zy_arrival = copies.arrivals(), copies.arrivals(2)

    def z_exchange_x():
        for i in range(2):
            src = wb.at[core, slot_x[3], 128 * i : 128 * i + 128, given]
            copies.start(src, zx.at[i], at(dz=1 - 2 * i), zx_group, zx_arrival)

    def z_exchange_y(k):
        for i in range(2):
            src = wb.at[core, 2 * k + 1, x_rows(0, i), given]
            copies.start(src, zy.at[k, i], at(dz=1 - 2 * i), zy_group, zy_arrival + min(k, 1))

    def z_add_x():
        copies.wait(zx, zx_arrival)
        for i in range(2):
            ref = wb.at[core, slot_x[3], 128 * i : 128 * i + 128, kept]
            ref[...] = ref[...] + zx[i]

    def z_add_y(first, n):
        copies.wait(zy.at[first : first + n], zy_arrival + min(first, 1))
        for k in range(first, first + n):
            for i in range(2):
                ref = wb.at[core, 2 * k + 1, x_rows(0, i), kept]
                ref[...] = ref[...] + zy[k, i]

    stage2 = (ring_x2, ring_y2)

    def pair_add(s):
        copies.wait(wd.at[s], pair + s)
        wb[core, s] = wb[core, s] + wd[s]

    def direct(ring):
        ring.direct_plus()
        ring.direct_minus()

    def accumulate(ring):
        ring.acc(0)
        ring.acc(1)

    def final_x(k):
        for h, v in enumerate(ring_x1[k].final()):
            if k == 3:
                own_sums[0, h, :, kept] = v
            else:
                wb[core, slot_x[k], x_rows(0, h)] = v

    def final_y(k):
        for h, v in enumerate(ring_y1[k].final()):
            if k == 3:
                own_sums[1, h, :, kept] = v
            else:
                wb[core, 7, x_rows(offsets[k], h)] = v

    phase("add0")
    pair_add(0)
    ring_x1[0].send2()
    direct(ring_x1[0])
    pl.semaphore_wait(know.at[0], 2)
    pl.semaphore_wait(know.at[3], 4)
    signal(know.at[4], at(dx=2))
    signal(know.at[4], at(dy=2))
    for d in (2, -2):
        signal(know.at[1], at(dz=d))
    phase("prod2")
    product(2)
    pair_send(2)
    phase("add12")
    pair_add(1)
    z_exchange_y(0)
    ring_y1[0].send2()
    ring_y1[1].send2()
    pair_add(2)
    ring_x1[1].send2()
    phase("prod3")
    product(3)
    pair_send(3)
    phase("add3")
    pair_add(3)
    z_exchange_y(1)
    ring_y1[2].send2()
    ring_y1[0].direct_plus()
    phase("bnpair")
    copies.wait(bnd, bn_pair)
    bnp[:, half] = bnp[:, half] + bnd[...]
    pl.semaphore_wait(know.at[4], 2)
    pl.semaphore_wait(know.at[1], 2)
    for d in (4, -4):
        signal(know.at[2], at(dz=d))

    def f_xy(dx, dy):
        start = mine + lax.rem(x + dx, NX) * F_X + lax.rem(y + dy, NY) * F_Y
        return pl.ds(mul(start, F_Y), F_Y)

    xy_group, xy = copies.group(bnx.at[1:16]), copies.arrivals()
    for dx, dy in plane:
        slot = bnx.at[4 * dx + dy]
        copies.start(bnp.at[:, f_xy(dx, dy)], slot, at(dx=dx, dy=dy), xy_group, xy)

    phase("add45")
    pair_add(4)
    z_exchange_x()
    pair_add(5)
    z_exchange_y(2)
    ring_y1[0].direct_minus()
    phase("acc0")
    accumulate(ring_x1[0])
    phase("add67")
    pair_add(6)
    ring_x1[2].send2()
    direct(ring_x1[1])
    pair_add(7)
    z_exchange_y(3)
    own_sums[...] = jnp.zeros_like(own_sums)
    phase("acc0y")
    accumulate(ring_y1[0])
    direct(ring_y1[1])
    def bn_z():
        copies.wait(bnx.at[1:16], xy)
        pl.semaphore_wait(know.at[2], 2)
        total = bnp[:, f_xy(0, 0)]
        for dx, dy in plane:
            total = total + bnx[4 * dx + dy]
        bnz[z] = total
        bz_group, bz = copies.group(bnz.at[0:15]), copies.arrivals()
        for d in far:
            copies.start(bnz.at[z], bnz.at[z], at(dz=d), bz_group, bz)
        return bz

    first, second = {"X": ring_x1, "Y": ring_y1}, {"X": ring_x2, "Y": ring_y2}
    finals = {"X": final_x, "Y": final_y}

    bz = None
    for step in " ".join(ORDER).split():
        phase(step)
        kind, c, k = step[0], step[1:2], int(step[2:3] or 0)
        if kind == "z":
            z_add_x() if c == "X" else z_add_y(0, 1)
            first[c][3].send2()
            continue
        if kind == "y":
            z_add_y(1, 3)
            continue
        if kind == "a":
            accumulate(first[c][k])
        elif kind == "d":
            direct(first[c][k])
        elif kind == "s":
            second[c].acc(k)
        elif kind == "f":
            finals[c](k)
            if k < 3:
                (second[c].send2, second[c].direct_plus, second[c].direct_minus)[k]()
        else:
            bz = bn_z()

    z_group, z_arrival = copies.group(zr.at[0:15]), copies.arrivals()

    def weight_z(colour):
        for h, v in enumerate(stage2[colour].final()):
            for i in range(2):
                zs[2 * colour + i, h * 32 : h * 32 + 32, :] = v[:, i * 128 : i * 128 + 128]
        for j in range(8):
            ll, hh = 2 * colour + j % 2, lax.rem(zh + offsets[j // 2], NZH)
            copy = copies.make(
                zs.at[ll, pl.ds(mul(hh * 16, 16), 16)],
                zr.at[z],
                (y * NZL + ll, (hh * NX + x) * 2 + core),
                z_group,
                z_arrival,
            )
            if j < 6:
                copy.start()
            else:
                pl.when(ll != zl)(copy.start)

    phase("wgtz0")
    weight_z(0)
    phase("wgtz1")
    weight_z(1)

    phase("bnz")
    copies.wait(bnz.at[0:15], bz)
    total = bnz[0]
    for i in range(1, NZ):
        total = total + bnz[i]
    own = bna.at[:, f_xy(0, 0)]
    own[...] = total * (1.0 / IMAGES)
    others = bna.at[:, 0 : 31 * F_Y]
    axy_group, axy = copies.group(others), copies.arrivals()
    for dx, dy in plane + [(0, 0)]:
        for dc in (1, 0):
            if dx or dy or dc:
                copies.start(own, own, at(dx=dx, dy=dy, dc=dc), axy_group, axy)
    zr[z] = zs[zl, pl.ds(mul(zh * 16, 16), 16)]

    phase("zwait")
    copies.wait(zr.at[0:15], z_arrival)
    result = zr[0]
    for i in range(1, NZ):
        result = result + zr[i]
    column = mul(zl // 2 * 1024 + y * W + lax.rem(zl, 2) * 128, 128)
    piece = wg.at[:, pl.ds(column, 128)]
    piece[...] = result * (1.0 / IMAGES)

    phase("ag")
    peers = [(2, 3), (2, 1), (2, 2), (1, 3), (3, 3), (1, 1), (3, 1), (1, 2), (3, 2)]
    peers += [(2, 0), (0, 3), (0, 1), (0, 2), (1, 0), (3, 0)]
    ag_group, ag = copies.group(zr.at[0:15]), copies.arrivals()
    for dy, dl in peers:
        device = (lax.rem(y + dy, NY) * NZL + lax.rem(zl + dl, NZL), zero)
        copies.start(piece, piece, device, ag_group, ag)

    phase("bngxy")
    copies.wait(others, axy)

    def grads(i, carry):
        cols = pl.ds(mul(i * 512, 512), 512)
        g = up[:, cols].astype(jnp.float32)
        n = (pre[:, cols].astype(jnp.float32) - mean[:, cols]) * inv[:, cols]
        scale = gain[:, cols] * inv[:, cols]
        bias_grad, gain_grad = bna[0:1, cols], bna[1:2, cols]
        bias_o[:, cols] = bias_grad
        gain_o[:, cols] = gain_grad
        ig[:, cols] = (scale * (g - bias_grad - n * gain_grad)).astype(jnp.bfloat16)
        return carry

    phase("grads")
    lax.fori_loop(0, F // 512, grads, 0)
    phase("agwait")
    copies.wait(zr.at[0:15], ag)
    phase("drain")
    copies.drain()
    phase(None)
    assert (len(copies.sends), copies.n_recv) == (N_SEND, N_RECV), "semaphore counts"


N_SEND, N_RECV = 11, 39
ORDER = (
    "aX1 dX2 aY1 aX2", "fX0 zY dY2 zX", "aY2 fY0 y b", "fX1 dX3 dY3 fY1",
    "aX3 aY3 sX0 sY0", "fX2 sX1 fY2 sY1", "fX3 fY3",
)


def store(ig, gain, bias, wg, ig_o, gain_o, bias_o, wg_o, sem):
    pairs = ((ig, ig_o), (wg, wg_o), (gain, gain_o), (bias, bias_o))
    copies = [pltpu.make_async_copy(a, b, sem.at[i]) for i, (a, b) in enumerate(pairs)]
    for copy in copies:
        copy.start()
    for copy in copies:
        copy.wait()


def per_device(pre_norm, upstream, norm_gain, saved_mean, inv_std, features, out_grads):
    row = lambda v: v.reshape(1, F)
    f32, bf16 = jnp.float32, jnp.bfloat16
    vm = pltpu.VMEM
    dma = pltpu.SemaphoreType.DMA
    outs = (
        jax.ShapeDtypeStruct((16, F), bf16),
        jax.ShapeDtypeStruct((1, F), f32),
        jax.ShapeDtypeStruct((1, F), f32),
        jax.ShapeDtypeStruct((16, COUT), f32),
    )
    vectors = (row(norm_gain), row(saved_mean), row(inv_std))
    arrays = (pre_norm, upstream, *vectors, features, out_grads)
    results = pl.pallas_call(
        kernel,
        out_shape=outs,
        in_specs=[pl.BlockSpec(memory_space=pltpu.HBM)] * 7,
        out_specs=(pl.BlockSpec(memory_space=vm),) * 4,
        scratch_shapes=[
            vm((2, 16, F), bf16), vm((3, 1, F), f32), vm((ROWS, CIN), bf16), vm((4, ROWS, 2 * W), bf16),
            vm((2, 8, 256, W), f32), vm((8, 256, W), f32),
            vm((8, 6, 32, W), f32), vm((2, 6, 32, W // 2), f32),
            vm((2, 128, W // 2), f32), vm((4, 2, 32, W // 2), f32), vm((2, 2, 32, W), f32),
            vm((NZL, 64, 128), f32), vm((NZ, 16, 128), f32),
            vm((2, F), f32), vm((2, F_CORE), f32), vm((16, 2, F_Y), f32),
            vm((NZ, 2, F_Y), f32), vm((2, F), f32),
            dma((7,)), dma((N_SEND,)), dma((N_RECV,)), pltpu.SemaphoreType.REGULAR((5,)),
        ],
        compiler_params=pltpu.CompilerParams(
            collective_id=0, has_side_effects=True, vmem_limit_bytes=32 * 1024 * 1024
        ),
        name="twins",
    )(*(pltpu.with_memory_space_constraint(v, pltpu.HBM) for v in arrays))
    ig, gain_grad, bias_grad, wg = pl.pallas_call(
        store,
        out_shape=outs,
        in_specs=[pl.BlockSpec(memory_space=pl.ANY)] * 4,
        out_specs=(pl.BlockSpec(memory_space=pltpu.HBM),) * 4,
        scratch_shapes=[dma((4,))],
        name="store",
    )(*(pltpu.with_memory_space_constraint(v, vm) for v in results))
    return ig, gain_grad.reshape(F), bias_grad.reshape(F), wg


def solution(mesh):
    split = P(("rep", "zero"), None)
    return jax.shard_map(
        per_device,
        mesh=mesh,
        in_specs=(split, split, P(), P(), P(), split, split),
        out_specs=(split, P(), P(), P("zero", None)),
        check_vma=False,
    )
```

```python
import functools

import jax
import jax.numpy as jnp
from jax import lax
from jax.experimental import pallas as pl
from jax.experimental.pallas import tpu as pltpu
from jax.sharding import PartitionSpec as P

MESH = pl.DeviceIdType.MESH
F = 8192
ROWS = 784
CIN = 512
COUT = 2048
IMAGES = 8192
NX, NY, NZL, NZH = 4, 4, 4, 4
NZ = NZL * NZH
W = 256
F_CORE, F_X, F_Y = F // 2, F // 8, F // 32


def mul(v, m):
    return pl.multiple_of(v, m)


class Phases:
    def __init__(self):
        self.open = None

    def __call__(self, name):
        if self.open is not None:
            self.open.__exit__(None, None, None)
        self.open = None
        if name is not None:
            self.open = jax.named_scope(name)
            self.open.__enter__()


class Copies:
    def __init__(self, send, recv, partner):
        self.send, self.recv, self.partner = send, recv, partner
        self.sends, self.n_recv = [], 0

    def group(self, whole):
        self.sends.append(whole)
        return len(self.sends) - 1

    def arrivals(self, n=1):
        self.n_recv += n
        return self.n_recv - n

    def make(self, src, dst, device, group, arrival):
        return pltpu.make_async_remote_copy(
            src_ref=src,
            dst_ref=dst,
            send_sem=self.send.at[group],
            recv_sem=self.recv.at[arrival],
            device_id=device,
            device_id_type=MESH,
        )

    def start(self, *args):
        self.make(*args).start()

    def wait(self, whole, arrival):
        self.make(whole, whole, self.partner, 0, arrival).wait_recv()

    def drain(self):
        for i, whole in enumerate(self.sends):
            self.make(whole, whole, self.partner, i, 0).wait_send()


class Ring4:
    def __init__(self, copies, group, src, bufs, plus, minus, split=False):
        self.c, self.group, self.src, self.bufs = copies, group, src, bufs
        self.plus, self.minus = plus, minus
        self.arrival = copies.arrivals(3 if split else 2)
        self.split = split

    def copy(self, ref, slot, device, arrival):
        self.c.start(ref, self.bufs.at[slot], device, self.group, self.arrival + arrival)

    def send2(self):
        self.copy(self.src(2, 0), 0, self.plus, 1)
        self.copy(self.src(2, 1), 1, self.minus, 2 if self.split else 1)

    def direct_plus(self):
        self.copy(self.src(1, 1), 3, self.plus, 0)

    def direct_minus(self):
        self.copy(self.src(3, 0), 2, self.minus, 0)

    def acc(self, half):
        if self.split:
            self.c.wait(self.bufs.at[half], self.arrival + 1 + half)
        elif half == 0:
            self.c.wait(self.bufs.at[0:2], self.arrival + 1)
        ref = self.src(1 if half == 0 else 3, half)
        ref[...] = ref[...] + self.bufs[half]
        self.copy(ref, 4 + half, self.plus if half == 0 else self.minus, 0)

    def final(self):
        self.c.wait(self.bufs.at[2:6], self.arrival)
        return [self.src(0, h)[...] + self.bufs[2 + h] + self.bufs[4 + h] for h in range(2)]


def kernel(
    pre_h, up_h, gain_h, mean_h, inv_h, feat_h, og_h,
    ig, gain_o, bias_o, wg,
    rows, vectors, feat, og,
    wb, wd, rings, half_rings, zx, zy, own_sums, zs, zr,
    bnp, bnd, bnx, bnz, bna,
    local_sem, send_sem, recv_sem, know,
):
    rep, zero = lax.axis_index("rep"), lax.axis_index("zero")
    y, zl = rep // NZL, lax.rem(rep, NZL)
    core = lax.rem(zero, 2)
    xq = zero // 2
    x, zh = lax.rem(xq, NX), xq // NX
    z = zh * NZL + zl

    def at(dx=0, dy=0, dz=0, dc=0):
        zz = lax.rem(z + dz + NZ, NZ)
        xx, yy = lax.rem(x + dx + NX, NX), lax.rem(y + dy + NY, NY)
        cc = lax.rem(core + dc, 2)
        return (yy * NZL + lax.rem(zz, NZL), (zz // NZL * NX + xx) * 2 + cc)

    phase = Phases()
    phase("start")
    offsets, own_early = (2, 1, 3, 0), (2, 1, 0, 3)
    slot_x = (0, 2, 6, 4)
    pltpu.make_async_copy(feat_h, feat, local_sem.at[4]).start()
    for k in range(4):
        for colour in range(2):
            off = (offsets, own_early)[colour == 0][k]
            column = mul(colour * 1024 + lax.rem(y + off, NY) * W, W)
            dst = og.at[k, :, colour * W : colour * W + W]
            pltpu.make_async_copy(og_h.at[:, pl.ds(column, W)], dst, local_sem.at[k]).start()
        if k == 1:
            pltpu.make_async_copy(up_h, rows.at[0], local_sem.at[5]).start()
            pltpu.make_async_copy(pre_h, rows.at[1], local_sem.at[5]).start()
            for i, v in enumerate((mean_h, inv_h, gain_h)):
                pltpu.make_async_copy(v, vectors.at[i], local_sem.at[6]).start()

    def loaded(ref, i):
        pltpu.make_async_remote_copy(
            src_ref=ref,
            dst_ref=ref,
            send_sem=local_sem.at[i],
            recv_sem=local_sem.at[i],
            device_id=at(dc=1),
            device_id_type=MESH,
        ).wait_recv()

    up, pre = rows.at[0], rows.at[1]
    mean, inv, gain = vectors.at[0], vectors.at[1], vectors.at[2]

    def signal(sem, device):
        pl.semaphore_signal(sem, inc=1, device_id=device, device_id_type=MESH)

    barrier = pltpu.get_barrier_semaphore()
    beside = [at(dx=1), at(dx=-1), at(dy=1), at(dy=-1)]
    near = [at(dc=1), at(dz=1), at(dz=-1)] + beside
    for device in near:
        signal(barrier, device)
    plane = [(2, 2), (2, 1), (2, 3), (1, 2), (3, 2), (1, 1), (1, 3), (3, 1), (3, 3)]
    plane += [(2, 0), (0, 2), (1, 0), (3, 0), (0, 1), (0, 3)]
    far = [8, 7, 9, 6, 10, 5, 11, 4, 12, 3, 13, 2, 14, 1, 15]

    copies = Copies(send_sem, recv_sem, at(dc=1))
    mine = core * F_CORE
    other = (1 - core) * F_CORE
    half = pl.ds(mul(mine, F_CORE), F_CORE)

    phase("featwait")
    loaded(feat, 4)

    def product(k):
        loaded(og.at[k], k)
        v = lax.dot_general(
            feat[...], og[k], (((0,), (0,)), ((), ())), preferred_element_type=jnp.float32
        )
        for c in range(2):
            for xx in range(NX):
                for zz in range(NZH):
                    dst = (xx * NZH + zz) * 16
                    src = ((zz * NX + xx) * 2 + c) * 16
                    for i in range(2):
                        wb[c, 2 * k + i, dst : dst + 16, :] = v[
                            src : src + 16, i * W : i * W + W
                        ]

    pair_group = copies.group(wd)
    pair = copies.arrivals(8)

    def pair_send(k):
        for s in (2 * k, 2 * k + 1):
            copies.start(wb.at[1 - core, s], wd.at[s], at(dc=1), pair_group, pair + s)

    phase("prod0")
    product(0)
    phase("barrier")
    pl.semaphore_wait(barrier, len(near))
    for device in beside:
        signal(know.at[3], device)
    for d in (1, -1):
        signal(know.at[0], at(dz=d))
    pair_send(0)
    phase("prod1")
    product(1)
    pair_send(1)
    phase("bnload")
    loaded(rows, 5)
    loaded(vectors, 6)

    def sums(i, carry):
        cols = pl.ds(mul(i * 512, 512), 512)
        g = up[:, cols].astype(jnp.float32)
        n = (pre[:, cols].astype(jnp.float32) - mean[:, cols]) * inv[:, cols]
        bnp[0:1, cols] = jnp.sum(g, axis=0, keepdims=True)
        bnp[1:2, cols] = jnp.sum(g * n, axis=0, keepdims=True)
        return carry

    phase("bnsum")
    lax.fori_loop(0, F // 512, sums, 0)
    bn_pair = copies.arrivals()
    copies.start(
        bnp.at[:, pl.ds(mul(other, F_CORE), F_CORE)], bnd, at(dc=1), copies.group(bnd), bn_pair
    )
    def x_rows(xx, h):
        return pl.ds(mul(lax.rem(x + xx, NX) * 64 + h * 32, 32), 32)

    order = {2: 0, 1: 1, 3: 2, 0: 3}
    ring_group, half_group = copies.group(rings), copies.group(half_rings)
    parity = lax.rem(zl, 2)
    kept = pl.ds(mul(parity * 128, 128), 128)
    given = pl.ds(mul((1 - parity) * 128, 128), 128)

    def bufs(k, colour):
        return half_rings.at[colour] if k == 3 else rings.at[3 * colour + k]

    def columns(k):
        return kept if k == 3 else slice(None)

    ring_x1 = [
        Ring4(
            copies,
            half_group if k == 3 else ring_group,
            lambda off, h, k=k: wb.at[core, slot_x[k], x_rows(off, h), columns(k)],
            bufs(k, 0),
            at(dx=1),
            at(dx=-1),
        )
        for k in range(4)
    ]
    ring_y1 = [
        Ring4(
            copies,
            half_group if k == 3 else ring_group,
            lambda off, h, k=k: wb.at[
                core, 2 * order[off] + 1, x_rows(offsets[k], h), columns(k)
            ],
            bufs(k, 1),
            at(dy=1),
            at(dy=-1),
        )
        for k in range(4)
    ]
    ring_x2 = Ring4(
        copies,
        ring_group,
        lambda off, h: (
            wb.at[core, slot_x[order[off]], x_rows(0, h)] if off else own_sums.at[0, h]
        ),
        rings.at[6],
        at(dy=1),
        at(dy=-1),
        split=True,
    )
    ring_y2 = Ring4(
        copies,
        ring_group,
        lambda off, h: wb.at[core, 7, x_rows(off, h)] if off else own_sums.at[1, h],
        rings.at[7],
        at(dx=1),
        at(dx=-1),
        split=True,
    )
    zx_group, zy_group = copies.group(zx), copies.group(zy)
    zx_arrival, zy_arrival = copies.arrivals(), copies.arrivals(2)

    def z_exchange_x():
        for i in range(2):
            src = wb.at[core, slot_x[3], 128 * i : 128 * i + 128, given]
            copies.start(src, zx.at[i], at(dz=1 - 2 * i), zx_group, zx_arrival)

    def z_exchange_y(k):
        for i in range(2):
            src = wb.at[core, 2 * k + 1, x_rows(0, i), given]
            copies.start(src, zy.at[k, i], at(dz=1 - 2 * i), zy_group, zy_arrival + min(k, 1))

    def z_add_x():
        copies.wait(zx, zx_arrival)
        for i in range(2):
            ref = wb.at[core, slot_x[3], 128 * i : 128 * i + 128, kept]
            ref[...] = ref[...] + zx[i]

    def z_add_y(first, n):
        copies.wait(zy.at[first : first + n], zy_arrival + min(first, 1))
        for k in range(first, first + n):
            for i in range(2):
                ref = wb.at[core, 2 * k + 1, x_rows(0, i), kept]
                ref[...] = ref[...] + zy[k, i]

    stage2 = (ring_x2, ring_y2)

    def pair_add(s):
        copies.wait(wd.at[s], pair + s)
        wb[core, s] = wb[core, s] + wd[s]

    def direct(ring):
        ring.direct_plus()
        ring.direct_minus()

    def accumulate(ring):
        ring.acc(0)
        ring.acc(1)

    def final_x(k):
        for h, v in enumerate(ring_x1[k].final()):
            if k == 3:
                own_sums[0, h, :, kept] = v
            else:
                wb[core, slot_x[k], x_rows(0, h)] = v

    def final_y(k):
        for h, v in enumerate(ring_y1[k].final()):
            if k == 3:
                own_sums[1, h, :, kept] = v
            else:
                wb[core, 7, x_rows(offsets[k], h)] = v

    phase("add0")
    pair_add(0)
    ring_x1[0].send2()
    direct(ring_x1[0])
    pl.semaphore_wait(know.at[0], 2)
    pl.semaphore_wait(know.at[3], 4)
    signal(know.at[4], at(dx=2))
    signal(know.at[4], at(dy=2))
    for d in (2, -2):
        signal(know.at[1], at(dz=d))
    phase("prod2")
    product(2)
    pair_send(2)
    phase("add12")
    pair_add(1)
    z_exchange_y(0)
    ring_y1[0].send2()
    ring_y1[1].send2()
    pair_add(2)
    ring_x1[1].send2()
    phase("prod3")
    product(3)
    pair_send(3)
    phase("add3")
    pair_add(3)
    z_exchange_y(1)
    ring_y1[2].send2()
    ring_y1[0].direct_plus()
    phase("bnpair")
    copies.wait(bnd, bn_pair)
    bnp[:, half] = bnp[:, half] + bnd[...]
    pl.semaphore_wait(know.at[4], 2)
    pl.semaphore_wait(know.at[1], 2)
    for d in (4, -4):
        signal(know.at[2], at(dz=d))

    def f_xy(dx, dy):
        start = mine + lax.rem(x + dx, NX) * F_X + lax.rem(y + dy, NY) * F_Y
        return pl.ds(mul(start, F_Y), F_Y)

    xy_group, xy = copies.group(bnx.at[1:16]), copies.arrivals()
    for dx, dy in plane:
        slot = bnx.at[4 * dx + dy]
        copies.start(bnp.at[:, f_xy(dx, dy)], slot, at(dx=dx, dy=dy), xy_group, xy)

    phase("add45")
    pair_add(4)
    z_exchange_x()
    pair_add(5)
    z_exchange_y(2)
    ring_y1[0].direct_minus()
    phase("acc0")
    accumulate(ring_x1[0])
    phase("add67")
    pair_add(6)
    ring_x1[2].send2()
    direct(ring_x1[1])
    pair_add(7)
    z_exchange_y(3)
    own_sums[...] = jnp.zeros_like(own_sums)
    phase("acc0y")
    accumulate(ring_y1[0])
    direct(ring_y1[1])
    def bn_z():
        copies.wait(bnx.at[1:16], xy)
        pl.semaphore_wait(know.at[2], 2)
        total = bnp[:, f_xy(0, 0)]
        for dx, dy in plane:
            total = total + bnx[4 * dx + dy]
        bnz[z] = total
        bz_group, bz = copies.group(bnz.at[0:15]), copies.arrivals()
        for d in far:
            copies.start(bnz.at[z], bnz.at[z], at(dz=d), bz_group, bz)
        return bz

    first, second = {"X": ring_x1, "Y": ring_y1}, {"X": ring_x2, "Y": ring_y2}
    finals = {"X": final_x, "Y": final_y}

    bz = None
    for step in " ".join(ORDER).split():
        phase(step)
        kind, c, k = step[0], step[1:2], int(step[2:3] or 0)
        if kind == "z":
            z_add_x() if c == "X" else z_add_y(0, 1)
            first[c][3].send2()
            continue
        if kind == "y":
            z_add_y(1, 3)
            continue
        if kind == "a":
            accumulate(first[c][k])
        elif kind == "d":
            direct(first[c][k])
        elif kind == "s":
            second[c].acc(k)
        elif kind == "f":
            finals[c](k)
            if k < 3:
                (second[c].send2, second[c].direct_plus, second[c].direct_minus)[k]()
        else:
            bz = bn_z()

    z_group, z_arrival = copies.group(zr.at[0:15]), copies.arrivals()

    def weight_z(colour):
        for h, v in enumerate(stage2[colour].final()):
            for i in range(2):
                zs[2 * colour + i, h * 32 : h * 32 + 32, :] = v[:, i * 128 : i * 128 + 128]
        for j in range(8):
            ll, hh = 2 * colour + j % 2, lax.rem(zh + offsets[j // 2], NZH)
            copy = copies.make(
                zs.at[ll, pl.ds(mul(hh * 16, 16), 16)],
                zr.at[z],
                (y * NZL + ll, (hh * NX + x) * 2 + core),
                z_group,
                z_arrival,
            )
            if j < 6:
                copy.start()
            else:
                pl.when(ll != zl)(copy.start)

    phase("wgtz0")
    weight_z(0)
    phase("wgtz1")
    weight_z(1)

    phase("bnz")
    copies.wait(bnz.at[0:15], bz)
    total = bnz[0]
    for i in range(1, NZ):
        total = total + bnz[i]
    own = bna.at[:, f_xy(0, 0)]
    own[...] = total * (1.0 / IMAGES)
    others = bna.at[:, 0 : 31 * F_Y]
    axy_group, axy = copies.group(others), copies.arrivals()
    for dx, dy in plane + [(0, 0)]:
        for dc in (1, 0):
            if dx or dy or dc:
                copies.start(own, own, at(dx=dx, dy=dy, dc=dc), axy_group, axy)
    zr[z] = zs[zl, pl.ds(mul(zh * 16, 16), 16)]

    phase("zwait")
    copies.wait(zr.at[0:15], z_arrival)
    result = zr[0]
    for i in range(1, NZ):
        result = result + zr[i]
    column = mul(zl // 2 * 1024 + y * W + lax.rem(zl, 2) * 128, 128)
    piece = wg.at[:, pl.ds(column, 128)]
    piece[...] = result * (1.0 / IMAGES)

    phase("ag")
    ag_group, ag = copies.group(zr.at[0:15]), copies.arrivals()
    far_first = [(2, 0), (1, 0), (3, 0), (2, 1), (0, 0), (1, 1), (3, 1), (2, 2), (0, 1)]
    far_first += [(1, 2), (3, 2), (2, 3), (0, 2), (1, 3), (3, 3), (0, 3)]
    for dy, i in far_first:
        to = i + (1 - zl // 2) * (3 - 2 * i)
        device = (lax.rem(y + dy, NY) * NZL + to, zero)
        copy = copies.make(piece, piece, device, ag_group, ag)
        if dy:
            copy.start()
        else:
            pl.when(to != zl)(copy.start)

    phase("bngxy")
    copies.wait(others, axy)

    def grads(i, carry):
        cols = pl.ds(mul(i * 512, 512), 512)
        g = up[:, cols].astype(jnp.float32)
        n = (pre[:, cols].astype(jnp.float32) - mean[:, cols]) * inv[:, cols]
        scale = gain[:, cols] * inv[:, cols]
        bias_grad, gain_grad = bna[0:1, cols], bna[1:2, cols]
        bias_o[:, cols] = bias_grad
        gain_o[:, cols] = gain_grad
        ig[:, cols] = (scale * (g - bias_grad - n * gain_grad)).astype(jnp.bfloat16)
        return carry

    phase("grads")
    lax.fori_loop(0, F // 512, grads, 0)
    phase("agwait")
    copies.wait(zr.at[0:15], ag)
    phase("drain")
    copies.drain()
    phase(None)
    assert (len(copies.sends), copies.n_recv) == (N_SEND, N_RECV), "semaphore counts"


N_SEND, N_RECV = 11, 39
ORDER = (
    "aX1 dX2 aY1 aX2", "fX0 zY dY2 zX", "aY2 fY0 y b", "fX1 dX3 dY3 fY1",
    "aX3 aY3 sX0 sY0", "fX2 sX1 fY2 sY1", "fX3 fY3",
)


def store(ig, gain, bias, wg, ig_o, gain_o, bias_o, wg_o, sem):
    pairs = ((ig, ig_o), (wg, wg_o), (gain, gain_o), (bias, bias_o))
    copies = [pltpu.make_async_copy(a, b, sem.at[i]) for i, (a, b) in enumerate(pairs)]
    for copy in copies:
        copy.start()
    for copy in copies:
        copy.wait()


def per_device(pre_norm, upstream, norm_gain, saved_mean, inv_std, features, out_grads):
    row = lambda v: v.reshape(1, F)
    f32, bf16 = jnp.float32, jnp.bfloat16
    vm = pltpu.VMEM
    dma = pltpu.SemaphoreType.DMA
    outs = (
        jax.ShapeDtypeStruct((16, F), bf16),
        jax.ShapeDtypeStruct((1, F), f32),
        jax.ShapeDtypeStruct((1, F), f32),
        jax.ShapeDtypeStruct((16, COUT), f32),
    )
    vectors = (row(norm_gain), row(saved_mean), row(inv_std))
    arrays = (pre_norm, upstream, *vectors, features, out_grads)
    results = pl.pallas_call(
        kernel,
        out_shape=outs,
        in_specs=[pl.BlockSpec(memory_space=pltpu.HBM)] * 7,
        out_specs=(pl.BlockSpec(memory_space=vm),) * 4,
        scratch_shapes=[
            vm((2, 16, F), bf16), vm((3, 1, F), f32), vm((ROWS, CIN), bf16), vm((4, ROWS, 2 * W), bf16),
            vm((2, 8, 256, W), f32), vm((8, 256, W), f32),
            vm((8, 6, 32, W), f32), vm((2, 6, 32, W // 2), f32),
            vm((2, 128, W // 2), f32), vm((4, 2, 32, W // 2), f32), vm((2, 2, 32, W), f32),
            vm((NZL, 64, 128), f32), vm((NZ, 16, 128), f32),
            vm((2, F), f32), vm((2, F_CORE), f32), vm((16, 2, F_Y), f32),
            vm((NZ, 2, F_Y), f32), vm((2, F), f32),
            dma((7,)), dma((N_SEND,)), dma((N_RECV,)), pltpu.SemaphoreType.REGULAR((5,)),
        ],
        compiler_params=pltpu.CompilerParams(
            collective_id=0, has_side_effects=True, vmem_limit_bytes=32 * 1024 * 1024
        ),
        name="twins",
    )(*(pltpu.with_memory_space_constraint(v, pltpu.HBM) for v in arrays))
    ig, gain_grad, bias_grad, wg = pl.pallas_call(
        store,
        out_shape=outs,
        in_specs=[pl.BlockSpec(memory_space=pl.ANY)] * 4,
        out_specs=(pl.BlockSpec(memory_space=pltpu.HBM),) * 4,
        scratch_shapes=[dma((4,))],
        name="store",
    )(*(pltpu.with_memory_space_constraint(v, vm) for v in results))
    return ig, gain_grad.reshape(F), bias_grad.reshape(F), wg


def solution(mesh):
    split = P(("rep", "zero"), None)
    return jax.shard_map(
        per_device,
        mesh=mesh,
        in_specs=(split, split, P(), P(), P(), split, split),
        out_specs=(split, P(), P(), P("zero", None)),
        check_vma=False,
    )
```
